128 devices in a mesh: section: 8 (over x, core), tp: 16 (over z, y).
Axes of the slice: x: 4, y: 4, z: 4, core: 2. Of those that a mesh axis runs over, the one named last changes fastest.
Arguments:
- pending_activation: bfloat16 [8, 128, 4096], P('section'), may hold values from -6 to 6
- admissible_microbatches: bfloat16 [4, 128, 4096], P(None, None, 'tp'), may hold values from -6 to 6
- arrival_plan: int32 [4], replicated, may hold values from 0 to 3, each once
- vanished_hop: int32 [1], replicated, may hold values from 1 to 7
- query_key_value_matrices: bfloat16 [8, 4096, 3, 2048], P('section', None, None, 'tp')
- mixing_projection_matrices: bfloat16 [8, 2048, 4096], P('section', 'tp'), may hold values from -0.125 to 0.125
- normalizer_factors: bfloat16 [8, 4096], P('section'), may hold values from 0.25 to 1.75
Outputs:
- activation_later: bfloat16 [8, 128, 4096], P('section')
- standby_input: bfloat16 [8, 128, 4096], P('section', None, 'tp')
The draws below stay inside these ranges and needn't reach their ends.
Inputs may be any that keep to these rules, and one draw needn't show every extreme that they name: `vanished_hop`: the preempted section is not the first. `arrival_plan`: each micro-batch index once.
All inputs are finite; a program needn't handle non-finite values.
Results may differ from the reference program's by a relative error of at most 0.013.
Values may be sent and summed in bfloat16 or wider, within the bound.
A program may use at most 64 MiB of HBM per device.

```python
import jax
import jax.numpy as jnp
from jax import lax

HIDDEN_SIZE = 4096
HEADS = 16
HD = 128
STRING_LENGTH = 128
TICKS = 3
POOL = 4
LAYER_HOPS = 8


def draw_query_key_value_matrices(key, part):
    base = jax.random.normal(key, (LAYER_HOPS, HIDDEN_SIZE, 3, HEADS * HD), jnp.float32) * HIDDEN_SIZE ** (-0.5)
    return base.astype(jnp.bfloat16)


def level_of(stream_key, dims, pieces, low, high):
    loudness = 1.0
    for position, shards_of in pieces:
        draws = jax.random.uniform(jax.random.fold_in(jax.random.fold_in(stream_key, 6), position), (shards_of,), jnp.float32, low / len(pieces), high / len(pieces))
        loudness = loudness * jnp.repeat(jnp.exp(draws), dims[position] // shards_of).reshape((-1,) + (1,) * (len(dims) - 1 - position))
    return loudness


def bell_draw(rng, dims, width, limit, cuts=(), held_as=jnp.bfloat16):
    array = jax.random.normal(rng, dims, jnp.float32) * width
    if len(cuts) > 0:
        array = level_of(rng, dims, cuts, -0.22, 0.18) * array
    return jnp.clip(array, min=-limit, max=limit).astype(held_as)


def setup_inputs(seed: int = 0) -> dict:
    arg_keys = jax.random.split(jax.random.key(seed), 8)
    pending_activation = bell_draw(arg_keys[0], (LAYER_HOPS, STRING_LENGTH, HIDDEN_SIZE), 1.0, 6.0, ((0, 8),))
    admissible_microbatches = bell_draw(arg_keys[1], (POOL, STRING_LENGTH, HIDDEN_SIZE), 1.0, 6.0, ((2, 16),))
    arrival_plan = jax.random.permutation(arg_keys[2], POOL).astype(jnp.int32)
    vanished_hop = jax.random.randint(arg_keys[3], (1,), 1, LAYER_HOPS).astype(jnp.int32)
    query_key_value_matrices = draw_query_key_value_matrices(jax.random.fold_in(arg_keys[7], 71), 0)
    mixing_projection_matrices = bell_draw(arg_keys[5], (LAYER_HOPS, HEADS * HD, HIDDEN_SIZE), (HEADS * HD) ** -0.5, 0.125, ((0, 8), (1, 16)))
    normalizer_factors = jnp.clip(1.0 + 0.15 * jax.random.normal(arg_keys[6], (LAYER_HOPS, HIDDEN_SIZE), jnp.float32), 0.25, 1.75).astype(jnp.bfloat16)
    return dict(pending_activation=pending_activation, admissible_microbatches=admissible_microbatches, arrival_plan=arrival_plan, vanished_hop=vanished_hop, query_key_value_matrices=query_key_value_matrices, mixing_projection_matrices=mixing_projection_matrices, normalizer_factors=normalizer_factors)


NORM_EPS = 1e-05

def layer_norm(x_rows, scale_row):
    widened = x_rows.astype(jnp.float32)
    row_mean = lax.optimization_barrier(jnp.mean(widened, axis=-1, keepdims=True))
    centered = widened - row_mean
    row_var = lax.optimization_barrier(jnp.mean(centered * centered, axis=-1, keepdims=True))
    return (centered * lax.rsqrt(row_var + NORM_EPS) * scale_row.astype(jnp.float32)).astype(jnp.bfloat16)

def attend(normed, w_in, w_out):
    row_count = normed.shape[0]
    col_count = w_in.shape[2]
    head_count = col_count // HD
    projected = jnp.dot(normed, w_in.reshape(w_in.shape[0], 3 * col_count), preferred_element_type=jnp.float32)
    projected = projected.astype(jnp.bfloat16).reshape(row_count, 3, head_count, HD)
    queries = projected[:, 0].astype(jnp.float32)
    key_rows = projected[:, 1].astype(jnp.float32)
    values = projected[:, 2].astype(jnp.float32)
    scores = jnp.einsum('qhd,khd->hqk', queries, key_rows) * HD ** (-0.5)
    causal = jnp.arange(row_count)[:, None] >= jnp.arange(row_count)[None, :]
    scores = jnp.where(causal[None], scores, -jnp.inf)
    row_max = lax.optimization_barrier(jnp.max(scores, axis=-1, keepdims=True))
    weights = jnp.exp(scores - row_max)
    probs = (weights / lax.optimization_barrier(jnp.sum(weights, axis=-1, keepdims=True))).astype(jnp.bfloat16)
    context = jnp.einsum('hqk,khd->qhd', probs.astype(jnp.float32), values)
    context = context.astype(jnp.bfloat16).reshape(row_count, col_count)
    return jnp.dot(context, w_out, preferred_element_type=jnp.float32)

def section_layer(x_rows, w_in, w_out, scale_row):
    branch = attend(layer_norm(x_rows, scale_row), w_in, w_out)
    return (x_rows.astype(jnp.float32) + branch).astype(jnp.bfloat16)

def reference(pending_activation, admissible_microbatches, arrival_plan, vanished_hop, query_key_value_matrices, mixing_projection_matrices, normalizer_factors):
    lost_at = vanished_hop[0]
    section_ids = jnp.arange(LAYER_HOPS)[:, None, None]
    activation_later = pending_activation
    spares = None
    for tick_index in range(TICKS):
        outputs = lax.map(lambda operands: section_layer(*operands), (activation_later, query_key_value_matrices, mixing_projection_matrices, normalizer_factors))
        if tick_index == TICKS - 1:
            spares = lax.map(lambda operands: section_layer(*operands), (outputs, jnp.roll(query_key_value_matrices, -1, axis=0), jnp.roll(mixing_projection_matrices, -1, axis=0), jnp.roll(normalizer_factors, -1, axis=0)))
            redone = lax.dynamic_index_in_dim(spares, lost_at - 1, 0, keepdims=False)
        else:
            earlier = lax.dynamic_index_in_dim(outputs, lost_at - 1, 0, keepdims=False)
            redone = section_layer(earlier, lax.dynamic_index_in_dim(query_key_value_matrices, lost_at, 0, keepdims=False), lax.dynamic_index_in_dim(mixing_projection_matrices, lost_at, 0, keepdims=False), lax.dynamic_index_in_dim(normalizer_factors, lost_at, 0, keepdims=False))
        outputs = lax.dynamic_update_index_in_dim(outputs, redone, lost_at - 1, 0)
        entering = lax.dynamic_index_in_dim(admissible_microbatches, arrival_plan[tick_index], 0, keepdims=True)
        shifted = jnp.concatenate([entering, outputs[:-1]], axis=0)
        activation_later = jnp.where(section_ids == lost_at, jnp.zeros_like(shifted), jnp.where(section_ids == lost_at + 1, redone[None], shifted))
    standby_input = jnp.roll(spares, 2, axis=0)
    return (activation_later, standby_input)
```

```python
import functools

import jax
import jax.numpy as jnp
from jax import lax
from jax.experimental import pallas as pl
from jax.experimental.pallas import tpu as pltpu
from jax.sharding import PartitionSpec as P

HD = 128
TICKS = 3
NORM_EPS = 1e-05
MESH = pl.DeviceIdType.MESH
WAVES = TICKS + 2
CHUNKS = 1
NEAR_FIRST = (1, 3, 2)


def relay_kernel(
    sections, nz, ny,
    lost_ref, plan_ref, pend_hbm, pool_hbm, win_hbm, wout_hbm, gain_ref,
    later_hbm, standby_ref,
    win_ref, colsum_ref, wout_ref, x_buf, b_buf, pool_ref, res_src, res_in, acc, s1, s2, qkv, ctx_own, ctx_in, stage,
    local_sem, ws, wr, xs, xr, c1s, c2s, cr, rs, rr,
):
    s = lax.axis_index("section")
    me = lax.axis_index("tp")
    z, y = me // ny, me % ny
    nxt, prv = (s + 1) % sections, (s + sections - 1) % sections
    devices = nz * ny
    total_rows, width = x_buf.shape[2], x_buf.shape[3]
    rows = total_rows // CHUNKS
    part = rows // 2
    cols = win_ref.shape[1] // 3
    group = ny * width
    lost = lost_ref[0]

    def at(dz, dy):
        return ((z + dz) % nz) * ny + (y + dy) % ny

    def row_of(dz):
        return (z + dz) % nz

    def copy_to(src, dst, send, recv, section, tp):
        return pltpu.make_async_remote_copy(
            src_ref=src, dst_ref=dst, send_sem=send, recv_sem=recv,
            device_id={"section": section, "tp": tp}, device_id_type=MESH,
        )

    def local(src, dst, i):
        return pltpu.make_async_copy(src, dst, local_sem.at[i])

    def pick(cond, a, b):
        return jnp.where(jnp.full(a.shape, cond), a, b)

    def runs(section, n):
        idle = (section == 0) & (n == TICKS)
        idle = idle | (((section == 1) | (section == 2)) & (n == TICKS + 1))
        return jnp.logical_not(idle)

    def gathers(section, n):
        return (n > 0) & jnp.logical_not((section == 1) & (n == TICKS + 1))

    for i in range(3):
        local(win_hbm.at[i], win_ref.at[:, pl.ds(i * cols, cols)], 0).start()
    for j in range(devices):
        local(pend_hbm.at[0, :, pl.ds(j * width, width)], x_buf.at[0, j], 1).start()
    local(pool_hbm, pool_ref, 2).start()

    barrier = pltpu.get_barrier_semaphore()
    for j in range(devices):
        pl.semaphore_signal(barrier, inc=1, device_id={"section": prv, "tp": j}, device_id_type=MESH)
    for k in range(1, nz):
        pl.semaphore_signal(barrier, inc=1, device_id={"section": s, "tp": at(k, 0)}, device_id_type=MESH)
    for k in range(1, ny):
        pl.semaphore_signal(barrier, inc=1, device_id={"section": s, "tp": at(0, k)}, device_id_type=MESH)
    pl.semaphore_wait(barrier, devices + nz + ny - 2)

    for dz in (0,) + NEAR_FIRST:
        for dy in (0,) + NEAR_FIRST:
            t = at(dz, dy)
            copy_to(wout_hbm.at[:, pl.ds(pl.multiple_of(t * width, 128), width)],
                    wout_ref.at[pl.ds(pl.multiple_of(me * cols, 128), cols)], ws, wr, nxt, t).start()

    pltpu.make_async_copy(win_ref, win_ref, local_sem.at[0]).wait()
    eye = lax.broadcasted_iota(jnp.int32, (width, width), 0) == lax.broadcasted_iota(jnp.int32, (width, width), 1)
    colsum_ref[...] = jnp.zeros_like(colsum_ref)

    def fold(j, carry):
        span = pl.ds(pl.multiple_of(j * width, width), width)
        scale = jnp.where(eye, jnp.broadcast_to(gain_ref[:, span].astype(jnp.float32), (width, width)), 0.0)
        scaled = jnp.dot(scale.astype(jnp.bfloat16), win_ref[span, :], preferred_element_type=jnp.float32)
        scaled = scaled.astype(jnp.bfloat16)
        win_ref[span, :] = scaled
        colsum_ref[...] += jnp.sum(scaled.astype(jnp.float32).reshape(width // 8, 8, 3 * cols), axis=0)
        return carry

    lax.fori_loop(0, devices, fold, 0)
    colsum_ref[...] = jnp.broadcast_to(jnp.sum(colsum_ref[...], axis=0, keepdims=True), colsum_ref.shape)
    pltpu.make_async_copy(x_buf.at[0], x_buf.at[0], local_sem.at[1]).wait()
    pltpu.make_async_copy(pool_ref, pool_ref, local_sem.at[2]).wait()
    own = x_buf[0, me]
    res_src[...] = pick(s == lost, jnp.zeros_like(own), own)

    def span_of(c):
        return pl.ds(c * rows, rows)

    def half_of(c, h):
        return pl.ds(c * rows + h * part, part)

    def residual(n, c, src):
        return copy_to(src, res_in.at[n, span_of(c)], rs.at[n, c], rr.at[n, c], nxt, me)

    for c in range(CHUNKS):
        residual(0, c, res_src.at[span_of(c)]).start()

    def x_copy(n, c, h, slot, tp):
        ref = x_buf.at[n, slot, half_of(c, h)]
        return copy_to(ref, ref, xs.at[n], xr.at[n, c, h, slot], s, tp)

    def x_send(n, c):
        for k in NEAR_FIRST:
            x_copy(n, c, 0, me, at(k, 0)).start()
            x_copy(n, c, 1, me, at(0, k)).start()
        for k in NEAR_FIRST:
            x_copy(n, c, 1, me, at(k, 0)).start()
            x_copy(n, c, 0, me, at(0, k)).start()

    def forward(copy, n, c, first):
        for k in first:
            copy(n, c, 0, at(k, 0), me).wait_recv()
            for m in NEAR_FIRST:
                copy(n, c, 0, at(k, 0), at(0, m)).start()
            copy(n, c, 1, at(0, k), me).wait_recv()
            for m in NEAR_FIRST:
                copy(n, c, 1, at(0, k), at(m, 0)).start()

    def settle(copy, n, c, dz):
        for k in (0,) + NEAR_FIRST:
            if k:
                copy(n, c, 0, at(dz, k), me).wait_recv()
            if dz:
                copy(n, c, 1, at(dz, k), me).wait_recv()

    def c_copy(n, c, h, slot, tp):
        ref = ctx_in.at[n, slot, half_of(c, h)]
        return copy_to(ref, ref, c2s.at[n], cr.at[n, c, h, slot], s, tp)

    def c_send(n, c):
        for k in (0,) + NEAR_FIRST:
            for h, tp in ((0, at(k, 0)), (1, at(0, k))):
                copy_to(ctx_own.at[n, half_of(c, h)], ctx_in.at[n, me, half_of(c, h)],
                        c1s.at[n], cr.at[n, c, h, me], nxt, tp).start()

    def layer(n, c):
        dead = (s == lost) & (n == 0)
        span = span_of(c)
        own = x_buf[n, me, span]
        own = pick(dead, jnp.zeros_like(own), own).astype(jnp.float32)
        shift = jnp.broadcast_to(jnp.sum(own, axis=-1, keepdims=True) / width, (rows, width))
        for i, dz in enumerate((0,) + NEAR_FIRST):
            @pl.when(n > 0)
            def _():
                settle(x_copy, n, c, dz)

            zr = row_of(dz)
            blocks, sums, squares = [], None, None
            for k in range(ny):
                block = x_buf[n, zr * ny + k, span]
                block = pick(dead, jnp.zeros_like(block), block)
                blocks.append(block)
                moved = block.astype(jnp.float32) - shift
                square = moved * moved
                sums = moved if sums is None else sums + moved
                squares = square if squares is None else squares + square
            wide = jnp.concatenate(blocks, axis=1)
            weights = win_ref[pl.ds(pl.multiple_of(zr * group, group), group), :]
            product = jnp.dot(wide, weights, preferred_element_type=jnp.float32)
            sums = sums[:, :width // 2] + sums[:, width // 2:]
            squares = squares[:, :width // 2] + squares[:, width // 2:]
            if i == 0:
                acc[...] = product
                s1[...] = sums
                s2[...] = squares
            elif i < nz - 1:
                acc[...] += product
                s1[...] += sums
                s2[...] += squares
            else:
                product = acc[...] + product
                sums = s1[...] + sums
                squares = s2[...] + squares
        count = float(devices * width)
        off = jnp.sum(sums, axis=-1, keepdims=True) / count
        var = jnp.sum(squares, axis=-1, keepdims=True) / count - off * off
        rstd = lax.rsqrt(var + NORM_EPS)
        mean = shift[:, :1] + off
        qkv[span] = ((product - mean * colsum_ref[:1]) * rstd).astype(jnp.bfloat16)
        seen = (c + 1) * rows
        q = qkv[span, :HD]
        k = qkv[:seen, HD:2 * HD]
        v = qkv[:seen, 2 * HD:]
        scores = lax.dot_general(q, k, (((1,), (1,)), ((), ())), preferred_element_type=jnp.float32)
        query = lax.broadcasted_iota(jnp.int32, (rows, seen), 0) + c * rows
        causal = query >= lax.broadcasted_iota(jnp.int32, (rows, seen), 1)
        scores = jnp.where(causal, scores * HD ** (-0.5), -jnp.inf)
        weights = jnp.exp(scores - jnp.max(scores, axis=-1, keepdims=True))
        probs = (weights / jnp.sum(weights, axis=-1, keepdims=True)).astype(jnp.bfloat16)
        ctx_own[n, span] = jnp.dot(probs, v, preferred_element_type=jnp.float32).astype(jnp.bfloat16)
        c_send(n, c)

    def finish(n, c):
        if c == 0:
            @pl.when(n == 0)
            def _():
                pltpu.make_async_copy(wout_ref, wout_ref, wr).wait()

        span = span_of(c)
        residual(n, c, res_src.at[span]).wait_recv()
        total = res_in[n, span].astype(jnp.float32)
        for dz in (0,) + NEAR_FIRST:
            settle(c_copy, n, c, dz)
            zr = row_of(dz)
            wide = jnp.concatenate([ctx_in[n, zr * ny + k, span] for k in range(ny)], axis=1)
            weights = wout_ref[pl.ds(pl.multiple_of(zr * ny * cols, ny * cols), ny * cols), :]
            total = total + jnp.dot(wide, weights, preferred_element_type=jnp.float32)
        b_buf[n + 1, span] = total.astype(jnp.bfloat16)

    def advance(n, c):
        span = span_of(c)

        @pl.when(s == 0)
        def _():
            settled = pick(sections - TICKS > lost, b_buf[TICKS, span], b_buf[TICKS + 1, span])
            settled = pick(sections - 1 == lost, b_buf[1, span], settled)
            x_buf[n + 1, me, span] = pick(n < TICKS, pool_ref[plan_ref[n], span], settled)

        @pl.when(s != 0)
        def _():
            x_buf[n + 1, me, span] = b_buf[n + 1, span]

        @pl.when(gathers(s, n + 1))
        def _():
            x_send(n + 1, c)

        @pl.when(runs(s, n + 1))
        def _():
            residual(n + 1, c, x_buf.at[n + 1, me, span]).start()

    def output():
        early = (s == 0) | (s < lost) | (s - TICKS > lost)
        for j in range(devices):
            block = pick(early, x_buf[TICKS, j], x_buf[TICKS + 1, j])
            stage[j] = pick(s == lost, jnp.zeros_like(block), block)
        for j in range(devices):
            local(stage.at[j], later_hbm.at[0, :, pl.ds(j * width, width)], 3).start()

    def step(n, carry):
        for c in range(CHUNKS):
            @pl.when(gathers(s, n))
            def _():
                forward(x_copy, n, c, NEAR_FIRST)

            if c:
                @pl.when(runs(prv, n))
                def _():
                    forward(c_copy, n, c - 1, (0,) + NEAR_FIRST)

            @pl.when(runs(s, n))
            def _():
                layer(n, c)

            @pl.when(gathers(s, n) & jnp.logical_not(runs(s, n)))
            def _():
                for dz in (0,) + NEAR_FIRST:
                    settle(x_copy, n, c, dz)

        @pl.when(n == WAVES - 1)
        def _():
            output()

        for c in range(CHUNKS):
            @pl.when(runs(prv, n))
            def _():
                if c == CHUNKS - 1:
                    forward(c_copy, n, c, (0,) + NEAR_FIRST)
                finish(n, c)

            @pl.when(jnp.logical_not(runs(prv, n)))
            def _():
                b_buf[n + 1, span_of(c)] = jnp.zeros((rows, width), jnp.bfloat16)

            @pl.when(n < WAVES - 1)
            def _():
                advance(n, c)

        return carry

    lax.fori_loop(0, WAVES, step, 0)

    settled = pick((s - 2 < lost) | (s - 2 - TICKS + 1 > lost), b_buf[TICKS + 1], b_buf[TICKS + 2])
    settled = pick((s + sections - 2) % sections == lost, b_buf[2], settled)
    last = sections - 2
    wrapped = pick((last < lost) | (last - TICKS + 1 > lost), b_buf[TICKS + 1], b_buf[TICKS + 2])
    wrapped = pick(last == lost, b_buf[2], wrapped)
    settled = pick(s == 0, wrapped, settled)
    standby_ref[0] = pick(s == 1, b_buf[TICKS + 2], settled)

    pltpu.make_async_copy(wout_ref, wout_ref, ws).wait()
    pltpu.make_async_copy(stage, stage, local_sem.at[3]).wait()

    def drain(n, carry):
        @pl.when(gathers(s, n))
        def _():
            ref = x_buf.at[0, pl.ds(0, devices - 1)]
            pltpu.make_async_copy(ref, ref, xs.at[n]).wait()

        @pl.when(runs(s, n))
        def _():
            ref = ctx_in.at[0, pl.ds(0, (nz + ny) // 2)]
            pltpu.make_async_copy(ref, ref, c1s.at[n]).wait()
            for c in range(CHUNKS):
                residual(n, c, res_src.at[span_of(c)]).wait_send()

        @pl.when(runs(prv, n))
        def _():
            ref = ctx_in.at[0, pl.ds(0, devices - (nz + ny) // 2)]
            pltpu.make_async_copy(ref, ref, c2s.at[n]).wait()

        return carry

    lax.fori_loop(0, WAVES, drain, 0)


def solution(mesh):
    sections, devices = mesh.shape["section"], mesh.shape["tp"]
    ny = 1
    while (2 * ny) * (2 * ny) <= devices and devices % (2 * ny) == 0:
        ny *= 2
    nz = devices // ny

    def per_device(pend, pool, plan, lost, win, wout, gain):
        rows, hidden = pend.shape[1], pend.shape[2]
        width = hidden // devices
        cols = win.shape[3]
        win = jnp.transpose(win[0], (1, 0, 2))
        vmem = pl.BlockSpec(memory_space=pltpu.VMEM)
        smem = pl.BlockSpec(memory_space=pltpu.SMEM)
        hbm = pl.BlockSpec(memory_space=pl.ANY)
        bf = functools.partial(pltpu.VMEM, dtype=jnp.bfloat16)
        f32 = functools.partial(pltpu.VMEM, dtype=jnp.float32)
        dma = pltpu.SemaphoreType.DMA
        chunk = rows // CHUNKS
        return pl.pallas_call(
            functools.partial(relay_kernel, sections, nz, ny),
            out_shape=(
                jax.ShapeDtypeStruct((1, rows, hidden), jnp.bfloat16),
                jax.ShapeDtypeStruct((1, rows, width), jnp.bfloat16),
            ),
            in_specs=[smem, smem, hbm, hbm, hbm, hbm, vmem],
            out_specs=(hbm, vmem),
            scratch_shapes=[
                bf((hidden, 3 * cols)),
                f32((8, 3 * cols)),
                bf((devices * cols, width)),
                bf((WAVES, devices, rows, width)),
                bf((WAVES + 1, rows, width)),
                bf(pool.shape),
                bf((rows, width)),
                bf((WAVES, rows, width)),
                f32((chunk, 3 * cols)),
                f32((chunk, width // 2)),
                f32((chunk, width // 2)),
                bf((rows, 3 * cols)),
                bf((WAVES, rows, cols)),
                bf((WAVES, devices, rows, cols)),
                bf((devices, rows, width)),
                dma((4,)), dma, dma,
                dma((WAVES,)), dma((WAVES, CHUNKS, 2, devices)),
                dma((WAVES,)), dma((WAVES,)), dma((WAVES, CHUNKS, 2, devices)),
                dma((WAVES, CHUNKS)), dma((WAVES, CHUNKS)),
            ],
            compiler_params=pltpu.CompilerParams(
                collective_id=0, has_side_effects=True, vmem_limit_bytes=60 * 1024 * 1024
            ),
        )(lost, plan, pend, pool, win, wout[0], gain)

    placed = (
        P("section", None, None),
        P(None, None, "tp"),
        P(),
        P(),
        P("section", None, None, "tp"),
        P("section", "tp", None),
        P("section", None),
    )
    return jax.shard_map(
        per_device,
        mesh=mesh,
        in_specs=placed,
        out_specs=(P("section", None, None), P("section", None, "tp")),
        check_vma=False,
    )
```

```python
import functools

import jax
import jax.numpy as jnp
from jax import lax
from jax.experimental import pallas as pl
from jax.experimental.pallas import tpu as pltpu
from jax.sharding import PartitionSpec as P

HD = 128
TICKS = 3
NORM_EPS = 1e-05
MESH = pl.DeviceIdType.MESH
WAVES = TICKS + 2
CHUNKS = 2
NEAR_FIRST = (1, 3, 2)


def relay_kernel(
    sections, nz, ny,
    lost_ref, plan_ref, pend_hbm, pool_hbm, win_hbm, wout_hbm, gain_ref,
    later_hbm, standby_ref,
    win_ref, colsum_ref, wout_ref, x_buf, b_buf, pool_ref, res_src, res_in, acc, s1, s2, qkv, ctx_own, ctx_in, stage,
    local_sem, ws, wr, xs, xr, c1s, c2s, cr, rs, rr,
):
    s = lax.axis_index("section")
    me = lax.axis_index("tp")
    z, y = me // ny, me % ny
    nxt, prv = (s + 1) % sections, (s + sections - 1) % sections
    devices = nz * ny
    total_rows, width = x_buf.shape[2], x_buf.shape[3]
    rows = total_rows // CHUNKS
    part = rows // 2
    cols = win_ref.shape[1] // 3
    group = ny * width
    lost = lost_ref[0]

    def at(dz, dy):
        return ((z + dz) % nz) * ny + (y + dy) % ny

    def row_of(dz):
        return (z + dz) % nz

    def copy_to(src, dst, send, recv, section, tp):
        return pltpu.make_async_remote_copy(
            src_ref=src, dst_ref=dst, send_sem=send, recv_sem=recv,
            device_id={"section": section, "tp": tp}, device_id_type=MESH,
        )

    def local(src, dst, i):
        return pltpu.make_async_copy(src, dst, local_sem.at[i])

    def pick(cond, a, b):
        return jnp.where(jnp.full(a.shape, cond), a, b)

    def runs(section, n):
        idle = (section == 0) & (n == TICKS)
        idle = idle | (((section == 1) | (section == 2)) & (n == TICKS + 1))
        return jnp.logical_not(idle)

    def gathers(section, n):
        return (n > 0) & jnp.logical_not((section == 1) & (n == TICKS + 1))

    for i in range(3):
        local(win_hbm.at[i], win_ref.at[:, pl.ds(i * cols, cols)], 0).start()
    for j in range(devices):
        local(pend_hbm.at[0, :, pl.ds(j * width, width)], x_buf.at[0, j], 1).start()
    local(pool_hbm, pool_ref, 2).start()

    barrier = pltpu.get_barrier_semaphore()
    for j in range(devices):
        pl.semaphore_signal(barrier, inc=1, device_id={"section": prv, "tp": j}, device_id_type=MESH)
    for k in range(1, nz):
        pl.semaphore_signal(barrier, inc=1, device_id={"section": s, "tp": at(k, 0)}, device_id_type=MESH)
    for k in range(1, ny):
        pl.semaphore_signal(barrier, inc=1, device_id={"section": s, "tp": at(0, k)}, device_id_type=MESH)
    pl.semaphore_wait(barrier, devices + nz + ny - 2)

    for dz in (0,) + NEAR_FIRST:
        for dy in (0,) + NEAR_FIRST:
            t = at(dz, dy)
            copy_to(wout_hbm.at[:, pl.ds(pl.multiple_of(t * width, 128), width)],
                    wout_ref.at[pl.ds(pl.multiple_of(me * cols, 128), cols)], ws, wr, nxt, t).start()

    pltpu.make_async_copy(win_ref, win_ref, local_sem.at[0]).wait()
    eye = lax.broadcasted_iota(jnp.int32, (width, width), 0) == lax.broadcasted_iota(jnp.int32, (width, width), 1)
    colsum_ref[...] = jnp.zeros_like(colsum_ref)

    def fold(j, carry):
        span = pl.ds(pl.multiple_of(j * width, width), width)
        scale = jnp.where(eye, jnp.broadcast_to(gain_ref[:, span].astype(jnp.float32), (width, width)), 0.0)
        scaled = jnp.dot(scale.astype(jnp.bfloat16), win_ref[span, :], preferred_element_type=jnp.float32)
        scaled = scaled.astype(jnp.bfloat16)
        win_ref[span, :] = scaled
        colsum_ref[...] += jnp.sum(scaled.astype(jnp.float32).reshape(width // 8, 8, 3 * cols), axis=0)
        return carry

    lax.fori_loop(0, devices, fold, 0)
    colsum_ref[...] = jnp.broadcast_to(jnp.sum(colsum_ref[...], axis=0, keepdims=True), colsum_ref.shape)
    pltpu.make_async_copy(x_buf.at[0], x_buf.at[0], local_sem.at[1]).wait()
    pltpu.make_async_copy(pool_ref, pool_ref, local_sem.at[2]).wait()
    own = x_buf[0, me]
    res_src[...] = pick(s == lost, jnp.zeros_like(own), own)

    def span_of(c):
        return pl.ds(c * rows, rows)

    def half_of(c, h):
        return pl.ds(c * rows + h * part, part)

    def residual(n, c, src):
        return copy_to(src, res_in.at[n, span_of(c)], rs.at[n, c], rr.at[n, c], nxt, me)

    for c in range(CHUNKS):
        residual(0, c, res_src.at[span_of(c)]).start()

    def x_copy(n, c, h, slot, tp):
        ref = x_buf.at[n, slot, half_of(c, h)]
        return copy_to(ref, ref, xs.at[n], xr.at[n, c, h, slot], s, tp)

    def x_send(n, c):
        for k in NEAR_FIRST:
            x_copy(n, c, 0, me, at(k, 0)).start()
            x_copy(n, c, 1, me, at(0, k)).start()
        for k in NEAR_FIRST:
            x_copy(n, c, 1, me, at(k, 0)).start()
            x_copy(n, c, 0, me, at(0, k)).start()

    def forward(copy, n, c, first):
        for k in first:
            copy(n, c, 0, at(k, 0), me).wait_recv()
            for m in NEAR_FIRST:
                copy(n, c, 0, at(k, 0), at(0, m)).start()
            copy(n, c, 1, at(0, k), me).wait_recv()
            for m in NEAR_FIRST:
                copy(n, c, 1, at(0, k), at(m, 0)).start()

    def settle(copy, n, c, dz):
        for k in (0,) + NEAR_FIRST:
            if k:
                copy(n, c, 0, at(dz, k), me).wait_recv()
            if dz:
                copy(n, c, 1, at(dz, k), me).wait_recv()

    def c_copy(n, c, h, slot, tp):
        ref = ctx_in.at[n, slot, half_of(c, h)]
        return copy_to(ref, ref, c2s.at[n], cr.at[n, c, h, slot], s, tp)

    def c_send(n, c):
        for k in (0,) + NEAR_FIRST:
            for h, tp in ((0, at(k, 0)), (1, at(0, k))):
                copy_to(ctx_own.at[n, half_of(c, h)], ctx_in.at[n, me, half_of(c, h)],
                        c1s.at[n], cr.at[n, c, h, me], nxt, tp).start()

    def layer(n, c):
        dead = (s == lost) & (n == 0)
        span = span_of(c)
        own = x_buf[n, me, span]
        own = pick(dead, jnp.zeros_like(own), own).astype(jnp.float32)
        shift = jnp.broadcast_to(jnp.sum(own, axis=-1, keepdims=True) / width, (rows, width))
        for i, dz in enumerate((0,) + NEAR_FIRST):
            @pl.when(n > 0)
            def _():
                settle(x_copy, n, c, dz)

            zr = row_of(dz)
            blocks, sums, squares = [], None, None
            for k in range(ny):
                block = x_buf[n, zr * ny + k, span]
                block = pick(dead, jnp.zeros_like(block), block)
                blocks.append(block)
                moved = block.astype(jnp.float32) - shift
                square = moved * moved
                sums = moved if sums is None else sums + moved
                squares = square if squares is None else squares + square
            wide = jnp.concatenate(blocks, axis=1)
            weights = win_ref[pl.ds(pl.multiple_of(zr * group, group), group), :]
            product = jnp.dot(wide, weights, preferred_element_type=jnp.float32)
            sums = sums[:, :width // 2] + sums[:, width // 2:]
            squares = squares[:, :width // 2] + squares[:, width // 2:]
            if i == 0:
                acc[...] = product
                s1[...] = sums
                s2[...] = squares
            elif i < nz - 1:
                acc[...] += product
                s1[...] += sums
                s2[...] += squares
            else:
                product = acc[...] + product
                sums = s1[...] + sums
                squares = s2[...] + squares
        count = float(devices * width)
        off = jnp.sum(sums, axis=-1, keepdims=True) / count
        var = jnp.sum(squares, axis=-1, keepdims=True) / count - off * off
        rstd = lax.rsqrt(var + NORM_EPS)
        mean = shift[:, :1] + off
        qkv[span] = ((product - mean * colsum_ref[:1]) * rstd).astype(jnp.bfloat16)
        seen = (c + 1) * rows
        q = qkv[span, :HD]
        k = qkv[:seen, HD:2 * HD]
        v = qkv[:seen, 2 * HD:]
        scores = lax.dot_general(q, k, (((1,), (1,)), ((), ())), preferred_element_type=jnp.float32)
        query = lax.broadcasted_iota(jnp.int32, (rows, seen), 0) + c * rows
        causal = query >= lax.broadcasted_iota(jnp.int32, (rows, seen), 1)
        scores = jnp.where(causal, scores * HD ** (-0.5), -jnp.inf)
        weights = jnp.exp(scores - jnp.max(scores, axis=-1, keepdims=True))
        probs = (weights / jnp.sum(weights, axis=-1, keepdims=True)).astype(jnp.bfloat16)
        ctx_own[n, span] = jnp.dot(probs, v, preferred_element_type=jnp.float32).astype(jnp.bfloat16)
        c_send(n, c)

    def finish(n, c):
        if c == 0:
            @pl.when(n == 0)
            def _():
                pltpu.make_async_copy(wout_ref, wout_ref, wr).wait()

        span = span_of(c)
        residual(n, c, res_src.at[span]).wait_recv()
        total = res_in[n, span].astype(jnp.float32)
        for dz in (0,) + NEAR_FIRST:
            settle(c_copy, n, c, dz)
            zr = row_of(dz)
            wide = jnp.concatenate([ctx_in[n, zr * ny + k, span] for k in range(ny)], axis=1)
            weights = wout_ref[pl.ds(pl.multiple_of(zr * ny * cols, ny * cols), ny * cols), :]
            total = total + jnp.dot(wide, weights, preferred_element_type=jnp.float32)
        b_buf[n + 1, span] = total.astype(jnp.bfloat16)

    def advance(n, c):
        span = span_of(c)

        @pl.when(s == 0)
        def _():
            settled = pick(sections - TICKS > lost, b_buf[TICKS, span], b_buf[TICKS + 1, span])
            settled = pick(sections - 1 == lost, b_buf[1, span], settled)
            x_buf[n + 1, me, span] = pick(n < TICKS, pool_ref[plan_ref[n], span], settled)

        @pl.when(s != 0)
        def _():
            x_buf[n + 1, me, span] = b_buf[n + 1, span]

        @pl.when(gathers(s, n + 1))
        def _():
            x_send(n + 1, c)

        @pl.when(runs(s, n + 1))
        def _():
            residual(n + 1, c, x_buf.at[n + 1, me, span]).start()

    def output():
        early = (s == 0) | (s < lost) | (s - TICKS > lost)
        for j in range(devices):
            block = pick(early, x_buf[TICKS, j], x_buf[TICKS + 1, j])
            stage[j] = pick(s == lost, jnp.zeros_like(block), block)
        for j in range(devices):
            local(stage.at[j], later_hbm.at[0, :, pl.ds(j * width, width)], 3).start()

    def step(n, carry):
        for c in range(CHUNKS):
            @pl.when(gathers(s, n))
            def _():
                forward(x_copy, n, c, NEAR_FIRST)

            if c:
                @pl.when(runs(prv, n))
                def _():
                    forward(c_copy, n, c - 1, (0,) + NEAR_FIRST)

            @pl.when(runs(s, n))
            def _():
                layer(n, c)

            @pl.when(gathers(s, n) & jnp.logical_not(runs(s, n)))
            def _():
                for dz in (0,) + NEAR_FIRST:
                    settle(x_copy, n, c, dz)

        @pl.when(n == WAVES - 1)
        def _():
            output()

        for c in range(CHUNKS):
            @pl.when(runs(prv, n))
            def _():
                if c == CHUNKS - 1:
                    forward(c_copy, n, c, (0,) + NEAR_FIRST)
                finish(n, c)

            @pl.when(jnp.logical_not(runs(prv, n)))
            def _():
                b_buf[n + 1, span_of(c)] = jnp.zeros((rows, width), jnp.bfloat16)

            @pl.when(n < WAVES - 1)
            def _():
                advance(n, c)

        return carry

    lax.fori_loop(0, WAVES, step, 0)

    settled = pick((s - 2 < lost) | (s - 2 - TICKS + 1 > lost), b_buf[TICKS + 1], b_buf[TICKS + 2])
    settled = pick((s + sections - 2) % sections == lost, b_buf[2], settled)
    last = sections - 2
    wrapped = pick((last < lost) | (last - TICKS + 1 > lost), b_buf[TICKS + 1], b_buf[TICKS + 2])
    wrapped = pick(last == lost, b_buf[2], wrapped)
    settled = pick(s == 0, wrapped, settled)
    standby_ref[0] = pick(s == 1, b_buf[TICKS + 2], settled)

    pltpu.make_async_copy(wout_ref, wout_ref, ws).wait()
    pltpu.make_async_copy(stage, stage, local_sem.at[3]).wait()

    def drain(n, carry):
        @pl.when(gathers(s, n))
        def _():
            ref = x_buf.at[0, pl.ds(0, devices - 1)]
            pltpu.make_async_copy(ref, ref, xs.at[n]).wait()

        @pl.when(runs(s, n))
        def _():
            ref = ctx_in.at[0, pl.ds(0, (nz + ny) // 2)]
            pltpu.make_async_copy(ref, ref, c1s.at[n]).wait()
            for c in range(CHUNKS):
                residual(n, c, res_src.at[span_of(c)]).wait_send()

        @pl.when(runs(prv, n))
        def _():
            ref = ctx_in.at[0, pl.ds(0, devices - (nz + ny) // 2)]
            pltpu.make_async_copy(ref, ref, c2s.at[n]).wait()

        return carry

    lax.fori_loop(0, WAVES, drain, 0)


def solution(mesh):
    sections, devices = mesh.shape["section"], mesh.shape["tp"]
    ny = 1
    while (2 * ny) * (2 * ny) <= devices and devices % (2 * ny) == 0:
        ny *= 2
    nz = devices // ny

    def per_device(pend, pool, plan, lost, win, wout, gain):
        rows, hidden = pend.shape[1], pend.shape[2]
        width = hidden // devices
        cols = win.shape[3]
        win = jnp.transpose(win[0], (1, 0, 2))
        vmem = pl.BlockSpec(memory_space=pltpu.VMEM)
        smem = pl.BlockSpec(memory_space=pltpu.SMEM)
        hbm = pl.BlockSpec(memory_space=pl.ANY)
        bf = functools.partial(pltpu.VMEM, dtype=jnp.bfloat16)
        f32 = functools.partial(pltpu.VMEM, dtype=jnp.float32)
        dma = pltpu.SemaphoreType.DMA
        chunk = rows // CHUNKS
        return pl.pallas_call(
            functools.partial(relay_kernel, sections, nz, ny),
            out_shape=(
                jax.ShapeDtypeStruct((1, rows, hidden), jnp.bfloat16),
                jax.ShapeDtypeStruct((1, rows, width), jnp.bfloat16),
            ),
            in_specs=[smem, smem, hbm, hbm, hbm, hbm, vmem],
            out_specs=(hbm, vmem),
            scratch_shapes=[
                bf((hidden, 3 * cols)),
                f32((8, 3 * cols)),
                bf((devices * cols, width)),
                bf((WAVES, devices, rows, width)),
                bf((WAVES + 1, rows, width)),
                bf(pool.shape),
                bf((rows, width)),
                bf((WAVES, rows, width)),
                f32((chunk, 3 * cols)),
                f32((chunk, width // 2)),
                f32((chunk, width // 2)),
                bf((rows, 3 * cols)),
                bf((WAVES, rows, cols)),
                bf((WAVES, devices, rows, cols)),
                bf((devices, rows, width)),
                dma((4,)), dma, dma,
                dma((WAVES,)), dma((WAVES, CHUNKS, 2, devices)),
                dma((WAVES,)), dma((WAVES,)), dma((WAVES, CHUNKS, 2, devices)),
                dma((WAVES, CHUNKS)), dma((WAVES, CHUNKS)),
            ],
            compiler_params=pltpu.CompilerParams(
                collective_id=0, has_side_effects=True, vmem_limit_bytes=60 * 1024 * 1024
            ),
        )(lost, plan, pend, pool, win, wout[0], gain)

    placed = (
        P("section", None, None),
        P(None, None, "tp"),
        P(),
        P(),
        P("section", None, None, "tp"),
        P("section", "tp", None),
        P("section", None),
    )
    return jax.shard_map(
        per_device,
        mesh=mesh,
        in_specs=placed,
        out_specs=(P("section", None, None), P("section", None, "tp")),
        check_vma=False,
    )
```

```python
import functools

import jax
import jax.numpy as jnp
from jax import lax
from jax.experimental import pallas as pl
from jax.experimental.pallas import tpu as pltpu
from jax.sharding import PartitionSpec as P

HD = 128
TICKS = 3
NORM_EPS = 1e-05
MESH = pl.DeviceIdType.MESH
WAVES = TICKS + 2
NEAR_FIRST = (1, 3, 2)
PEERS = tuple((k, 0) for k in NEAR_FIRST) + tuple((0, k) for k in NEAR_FIRST)


def relay_kernel(
    sections, nz, ny,
    lost_ref, plan_ref, pend_hbm, pool_hbm, win_hbm, wout_hbm, gain_hbm,
    later_hbm, standby_ref,
    win_ref, gain_ref, colsum_ref, wsrc_ref, wout_ref, x_buf, b_buf, pool_ref, res_src, res_in, acc, s1, s2, own_sum, ctx_in, sums_out, sums_in, stage,
    local_sem, ws, wr, xs, xr, cs, cr, ps, pr, rs, rr,
):
    s = lax.axis_index("section")
    me = lax.axis_index("tp")
    z, y = me // ny, me % ny
    nxt, prv = (s + 1) % sections, (s + sections - 1) % sections
    devices = nz * ny
    rows, width = x_buf.shape[2], x_buf.shape[3]
    half = rows // 2
    cols = win_ref.shape[1] // 3
    group = ny * width
    lost = lost_ref[0]

    def at(dz, dy):
        return ((z + dz) % nz) * ny + (y + dy) % ny

    def row_of(dz):
        return (z + dz) % nz

    def copy_to(src, dst, send, recv, section, tp):
        return pltpu.make_async_remote_copy(
            src_ref=src, dst_ref=dst, send_sem=send, recv_sem=recv,
            device_id={"section": section, "tp": tp}, device_id_type=MESH,
        )

    def local(src, dst, i):
        return pltpu.make_async_copy(src, dst, local_sem.at[i])

    def pick(cond, a, b):
        return jnp.where(jnp.full(a.shape, cond), a, b)

    def runs(section, n):
        idle = (section == 0) & (n == TICKS)
        idle = idle | (((section == 1) | (section == 2)) & (n == TICKS + 1))
        return jnp.logical_not(idle)

    def gathers(section, n):
        return (n > 0) & jnp.logical_not((section == 1) & (n == TICKS + 1))

    local(gain_hbm, gain_ref, 4).start()
    for i in range(3):
        local(win_hbm.at[i], win_ref.at[:, pl.ds(i * cols, cols)], 0).start()
    for j in range(devices):
        local(pend_hbm.at[0, :, pl.ds(j * width, width)], x_buf.at[0, j], 1).start()
    local(wout_hbm, wsrc_ref, 5).start()
    for j in range(nz):
        local(wout_hbm.at[:, pl.ds(pl.multiple_of((j * ny + y) * width, 128), width // 2)],
              wout_ref.at[0, pl.ds(pl.multiple_of(y * cols, 128), cols), pl.ds(j * (width // 2), width // 2)], 6).start()
    local(pool_hbm, pool_ref, 2).start()

    barrier = pltpu.get_barrier_semaphore()
    for dz, dy in PEERS + ((0, 0),):
        pl.semaphore_signal(barrier, inc=1, device_id={"section": prv, "tp": at(dz, dy)}, device_id_type=MESH)
    for dz, dy in PEERS:
        pl.semaphore_signal(barrier, inc=1, device_id={"section": s, "tp": at(dz, dy)}, device_id_type=MESH)

    eye = lax.broadcasted_iota(jnp.int32, (width, width), 0) == lax.broadcasted_iota(jnp.int32, (width, width), 1)
    colsum_ref[...] = jnp.zeros_like(colsum_ref)
    local(gain_hbm, gain_ref, 4).wait()
    pltpu.make_async_copy(win_ref, win_ref, local_sem.at[0]).wait()

    def fold(j, carry):
        span = pl.ds(pl.multiple_of(j * width, width), width)
        scale = jnp.where(eye, jnp.broadcast_to(gain_ref[:, span].astype(jnp.float32), (width, width)), 0.0)
        scaled = jnp.dot(scale.astype(jnp.bfloat16), win_ref[span, :], preferred_element_type=jnp.float32)
        scaled = scaled.astype(jnp.bfloat16)
        win_ref[span, :] = scaled
        colsum_ref[...] += jnp.sum(scaled.astype(jnp.float32).reshape(width // 8, 8, 3 * cols), axis=0)
        return carry

    with jax.named_scope("fold"):
        lax.fori_loop(0, devices, fold, 0, unroll=4)
    colsum_ref[...] = jnp.broadcast_to(jnp.sum(colsum_ref[...], axis=0, keepdims=True), colsum_ref.shape)
    pltpu.make_async_copy(x_buf.at[0], x_buf.at[0], local_sem.at[1]).wait()
    own = x_buf[0, me]
    res_src[...] = pick(s == lost, jnp.zeros_like(own), own)

    def residual(n, src):
        return copy_to(src, res_in.at[n], rs.at[n], rr.at[n], nxt, me)

    def w_send():
        for k in (2, 1, 3, 0):
            for j in range(ny):
                t = row_of(k) * ny + j
                copy_to(wsrc_ref.at[:, pl.ds(pl.multiple_of(t * width + width // 2, 128), width // 2)],
                        wout_ref.at[1, pl.ds(pl.multiple_of(z * cols, 128), cols), pl.ds(j * (width // 2), width // 2)],
                        ws, wr.at[1], nxt, at(k, 0)).start()
            if k:
                for j in range(nz):
                    t = j * ny + (y + k) % ny
                    copy_to(wsrc_ref.at[:, pl.ds(pl.multiple_of(t * width, 128), width // 2)],
                            wout_ref.at[0, pl.ds(pl.multiple_of(y * cols, 128), cols), pl.ds(j * (width // 2), width // 2)],
                            ws, wr.at[0], s, at(0, k)).start()

    def half_of(h):
        return pl.ds(h * half, half)

    def x_copy(n, h, slot, tp):
        ref = x_buf.at[n, slot, half_of(h)]
        return copy_to(ref, ref, xs.at[n], xr.at[n, h, slot], s, tp)

    def x_send(n):
        for k in NEAR_FIRST:
            x_copy(n, 0, me, at(k, 0)).start()
            x_copy(n, 1, me, at(0, k)).start()
        for k in NEAR_FIRST:
            x_copy(n, 1, me, at(k, 0)).start()
            x_copy(n, 0, me, at(0, k)).start()

    def x_forward(n):
        for k in NEAR_FIRST:
            x_copy(n, 0, at(k, 0), me).wait_recv()
            for m in NEAR_FIRST:
                x_copy(n, 0, at(k, 0), at(0, m)).start()
            x_copy(n, 1, at(0, k), me).wait_recv()
            for m in NEAR_FIRST:
                x_copy(n, 1, at(0, k), at(m, 0)).start()

    def x_settle(n, dz):
        for k in (0,) + NEAR_FIRST:
            if k:
                x_copy(n, 0, at(dz, k), me).wait_recv()
            if dz:
                x_copy(n, 1, at(dz, k), me).wait_recv()

    def c_copy(n, slot, section, tp):
        return copy_to(ctx_in.at[n, y], ctx_in.at[n, slot], cs.at[n], cr.at[n, slot], section, tp)

    def c_send(n):
        for k in (2, 1, 3, 0):
            c_copy(n, ny + z, nxt, at(k, 0)).start()
            if k:
                c_copy(n, y, s, at(0, k)).start()

    def p_copy(n, i, k, j, section, tp):
        return copy_to(sums_out.at[n, i, j], sums_in.at[n, i, k], ps.at[n, i], pr.at[n, i, k], section, tp)

    def partial(n, i):
        heads = jnp.concatenate([ctx_in[n, i * ny + k] for k in range(ny)], axis=1)
        sums = jnp.dot(heads, wout_ref[i], preferred_element_type=jnp.float32)
        for j in range(nz):
            piece = sums[:, j * (width // 2):(j + 1) * (width // 2)]
            if i:
                own_sum[j] = piece
            sums_out[n, i, j] = piece.astype(jnp.bfloat16)

    def spread(n):
        with jax.named_scope("cwait0"):
            for k in NEAR_FIRST:
                c_copy(n, (y + k) % ny, s, me).wait_recv()
        partial(n, 0)
        for k in (2, 1, 3, 0):
            p_copy(n, 0, k, row_of(k), nxt, at(k, 0)).start()

    def layer(n, first):
        def alive(block):
            return pick(s == lost, jnp.zeros_like(block), block) if first else block

        own = alive(x_buf[n, me]).astype(jnp.float32)
        shift = jnp.broadcast_to(jnp.sum(own, axis=-1, keepdims=True) / width, (rows, width))
        for i, dz in enumerate((0,) + NEAR_FIRST):
            if not first:
                with jax.named_scope("xsettle%d" % i):
                    x_settle(n, dz)
            zr = row_of(dz)
            blocks, sums, squares = [], None, None
            for k in range(ny):
                block = alive(x_buf[n, zr * ny + k])
                blocks.append(block)
                moved = block.astype(jnp.float32) - shift
                square = moved * moved
                sums = moved if sums is None else sums + moved
                squares = square if squares is None else squares + square
            wide = jnp.concatenate(blocks, axis=1)
            weights = win_ref[pl.ds(pl.multiple_of(zr * group, group), group), :]
            product = jnp.dot(wide, weights, preferred_element_type=jnp.float32)
            sums = sums[:, :width // 2] + sums[:, width // 2:]
            squares = squares[:, :width // 2] + squares[:, width // 2:]
            if i == 0:
                acc[...] = product
                s1[...] = sums
                s2[...] = squares
            elif i < nz - 1:
                acc[...] += product
                s1[...] += sums
                s2[...] += squares
            else:
                product = acc[...] + product
                sums = s1[...] + sums
                squares = s2[...] + squares
        with jax.named_scope("attend"):
            attend(n, product, sums, squares, shift)

    def attend(n, product, sums, squares, shift):
        count = float(devices * width)
        off = jnp.sum(sums, axis=-1, keepdims=True) / count
        var = jnp.sum(squares, axis=-1, keepdims=True) / count - off * off
        rstd = lax.rsqrt(var + NORM_EPS)
        mean = shift[:, :1] + off
        qkv = ((product - mean * colsum_ref[:1]) * rstd).astype(jnp.bfloat16)
        q, k, v = qkv[:, :HD], qkv[:, HD:2 * HD], qkv[:, 2 * HD:]
        scores = lax.dot_general(q, k, (((1,), (1,)), ((), ())), preferred_element_type=jnp.float32)
        causal = lax.broadcasted_iota(jnp.int32, (rows, rows), 0) >= lax.broadcasted_iota(jnp.int32, (rows, rows), 1)
        scores = jnp.where(causal, scores * HD ** (-0.5), -jnp.inf)
        weights = jnp.exp(scores - jnp.max(scores, axis=-1, keepdims=True))
        probs = (weights / jnp.sum(weights, axis=-1, keepdims=True)).astype(jnp.bfloat16)
        ctx_in[n, y] = jnp.dot(probs, v, preferred_element_type=jnp.float32).astype(jnp.bfloat16)

    def finish(n):
        with jax.named_scope("cwait1"):
            for k in (0,) + NEAR_FIRST:
                c_copy(n, ny + row_of(k), s, me).wait_recv()
        partial(n, 1)
        for k in (2, 1, 3):
            p_copy(n, 1, k, (y + k) % ny, s, at(0, k)).start()
        residual(n, res_src).wait_recv()
        for i in (1, 0):
            at_i = slice(i * (width // 2), (i + 1) * (width // 2))
            total = res_in[n, :, at_i].astype(jnp.float32)
            if i:
                total = total + own_sum[y]
            with jax.named_scope("pwait%d" % i):
                for k in NEAR_FIRST + ((0,) if i == 0 else ()):
                    p_copy(n, i, k, 0, s, me).wait_recv()
            for k in NEAR_FIRST + ((0,) if i == 0 else ()):
                total = total + sums_in[n, i, k].astype(jnp.float32)
            b_buf[n + 1, :, at_i] = total.astype(jnp.bfloat16)

    def advance(n):
        @pl.when(s == 0)
        def _():
            settled = pick(sections - TICKS > lost, b_buf[TICKS], b_buf[TICKS + 1])
            settled = pick(sections - 1 == lost, b_buf[1], settled)
            x_buf[n + 1, me] = pick(n < TICKS, pool_ref[plan_ref[n]], settled)

        @pl.when(s != 0)
        def _():
            x_buf[n + 1, me] = b_buf[n + 1]

        @pl.when(gathers(s, n + 1))
        def _():
            x_send(n + 1)

        @pl.when(runs(s, n + 1))
        def _():
            residual(n + 1, x_buf.at[n + 1, me]).start()

    def output():
        early = (s == 0) | (s < lost) | (s - TICKS > lost)
        for j in range(devices):
            block = pick(early, x_buf[TICKS, j], x_buf[TICKS + 1, j])
            stage[j] = pick(s == lost, jnp.zeros_like(block), block)
        for j in range(devices):
            local(stage.at[j], later_hbm.at[0, :, pl.ds(j * width, width)], 3).start()

    pltpu.make_async_copy(wsrc_ref, wsrc_ref, local_sem.at[5]).wait()
    with jax.named_scope("bwait"):
        pl.semaphore_wait(barrier, 2 * len(PEERS) + 1)
    w_send()
    layer(0, True)
    c_send(0)
    residual(0, res_src).start()
    pltpu.make_async_copy(pool_ref, pool_ref, local_sem.at[2]).wait()
    with jax.named_scope("wwait"):
        took = wout_ref.at[0, pl.ds(0, cols)]
        pltpu.make_async_copy(took, took, local_sem.at[6]).wait()
        took = x_buf.at[0, pl.ds(0, devices * (ny - 1) // 8)]
        pltpu.make_async_copy(took, took, wr.at[0]).wait()
        pltpu.make_async_copy(wout_ref.at[1], wout_ref.at[1], wr.at[1]).wait()

    def step(n, carry):
        @pl.when(gathers(s, n))
        def _():
            with jax.named_scope("xfwd"):
                x_forward(n)

        @pl.when(runs(s, n) & (n > 0))
        def _():
            layer(n, False)
            with jax.named_scope("csend"):
                c_send(n)

        @pl.when(runs(s, n))
        def _():
            with jax.named_scope("spread"):
                spread(n)

        @pl.when(gathers(s, n) & jnp.logical_not(runs(s, n)))
        def _():
            for dz in (0,) + NEAR_FIRST:
                x_settle(n, dz)

        @pl.when(n == WAVES - 1)
        def _():
            with jax.named_scope("output"):
                output()

        @pl.when(runs(prv, n))
        def _():
            with jax.named_scope("finish"):
                finish(n)

        @pl.when(jnp.logical_not(runs(prv, n)))
        def _():
            b_buf[n + 1] = jnp.zeros((rows, width), jnp.bfloat16)

        @pl.when(n < WAVES - 1)
        def _():
            with jax.named_scope("advance"):
                advance(n)

        return carry

    lax.fori_loop(0, WAVES, step, 0)

    settled = pick((s - 2 < lost) | (s - 2 - TICKS + 1 > lost), b_buf[TICKS + 1], b_buf[TICKS + 2])
    settled = pick((s + sections - 2) % sections == lost, b_buf[2], settled)
    last = sections - 2
    wrapped = pick((last < lost) | (last - TICKS + 1 > lost), b_buf[TICKS + 1], b_buf[TICKS + 2])
    wrapped = pick(last == lost, b_buf[2], wrapped)
    settled = pick(s == 0, wrapped, settled)
    standby_ref[0] = pick(s == 1, b_buf[TICKS + 2], settled)

    sent = x_buf.at[0, pl.ds(0, devices * (2 * ny - 1) // 8)]
    pltpu.make_async_copy(sent, sent, ws).wait()
    pltpu.make_async_copy(stage, stage, local_sem.at[3]).wait()

    def drain(n, carry):
        @pl.when(gathers(s, n))
        def _():
            ref = x_buf.at[0, pl.ds(0, devices - 1)]
            pltpu.make_async_copy(ref, ref, xs.at[n]).wait()

        @pl.when(runs(s, n))
        def _():
            ref = ctx_in.at[0, pl.ds(0, nz + ny - 1)]
            pltpu.make_async_copy(ref, ref, cs.at[n]).wait()
            ref = ctx_in.at[0, pl.ds(0, nz)]
            pltpu.make_async_copy(ref, ref, ps.at[n, 0]).wait()
            residual(n, res_src).wait_send()

        @pl.when(runs(prv, n))
        def _():
            ref = ctx_in.at[0, pl.ds(0, ny - 1)]
            pltpu.make_async_copy(ref, ref, ps.at[n, 1]).wait()

        return carry

    with jax.named_scope("drain"):
        lax.fori_loop(0, WAVES, drain, 0)


def solution(mesh):
    sections, devices = mesh.shape["section"], mesh.shape["tp"]
    ny = 1
    while (2 * ny) * (2 * ny) <= devices and devices % (2 * ny) == 0:
        ny *= 2
    nz = devices // ny

    def per_device(pend, pool, plan, lost, win, wout, gain):
        rows, hidden = pend.shape[1], pend.shape[2]
        width = hidden // devices
        cols = win.shape[3]
        win = jnp.transpose(win[0], (1, 0, 2))
        vmem = pl.BlockSpec(memory_space=pltpu.VMEM)
        smem = pl.BlockSpec(memory_space=pltpu.SMEM)
        hbm = pl.BlockSpec(memory_space=pl.ANY)
        bf = functools.partial(pltpu.VMEM, dtype=jnp.bfloat16)
        f32 = functools.partial(pltpu.VMEM, dtype=jnp.float32)
        dma = pltpu.SemaphoreType.DMA
        return pl.pallas_call(
            functools.partial(relay_kernel, sections, nz, ny),
            out_shape=(
                jax.ShapeDtypeStruct((1, rows, hidden), jnp.bfloat16),
                jax.ShapeDtypeStruct((1, rows, width), jnp.bfloat16),
            ),
            in_specs=[smem, smem, hbm, hbm, hbm, hbm, hbm],
            out_specs=(hbm, vmem),
            scratch_shapes=[
                bf((hidden, 3 * cols)),
                bf(gain.shape),
                f32((8, 3 * cols)),
                bf((cols, hidden)),
                bf((2, ny * cols, nz * width // 2)),
                bf((WAVES, devices, rows, width)),
                bf((WAVES + 1, rows, width)),
                bf(pool.shape),
                bf((rows, width)),
                bf((WAVES, rows, width)),
                f32((rows, 3 * cols)),
                f32((rows, width // 2)),
                f32((rows, width // 2)),
                f32((ny, rows, width // 2)),
                bf((WAVES, nz + ny, rows, cols)),
                bf((WAVES, 2, nz, rows, width // 2)),
                bf((WAVES, 2, nz, rows, width // 2)),
                bf((devices, rows, width)),
                dma((7,)), dma, dma((2,)),
                dma((WAVES,)), dma((WAVES, 2, devices)),
                dma((WAVES,)), dma((WAVES, nz + ny)),
                dma((WAVES, 2)), dma((WAVES, 2, nz)),
                dma((WAVES,)), dma((WAVES,)),
            ],
            compiler_params=pltpu.CompilerParams(
                collective_id=0, has_side_effects=True, vmem_limit_bytes=60 * 1024 * 1024
            ),
        )(lost, plan, pend, pool, win, wout[0], gain)

    placed = (
        P("section", None, None),
        P(None, None, "tp"),
        P(),
        P(),
        P("section", None, None, "tp"),
        P("section", "tp", None),
        P("section", None),
    )
    return jax.shard_map(
        per_device,
        mesh=mesh,
        in_specs=placed,
        out_specs=(P("section", None, None), P("section", None, "tp")),
        check_vma=False,
    )
```

```python
import functools

import jax
import jax.numpy as jnp
from jax import lax
from jax.experimental import pallas as pl
from jax.experimental.pallas import tpu as pltpu
from jax.sharding import PartitionSpec as P

HD = 128
TICKS = 3
NORM_EPS = 1e-05
MESH = pl.DeviceIdType.MESH
WAVES = TICKS + 2
NEAR_FIRST = (1, 3, 2)
PEERS = tuple((k, 0) for k in NEAR_FIRST) + tuple((0, k) for k in NEAR_FIRST)


def relay_kernel(
    sections, nz, ny,
    lost_ref, plan_ref, pend_hbm, pool_hbm, win_hbm, wout_hbm, gain_hbm,
    later_hbm, standby_ref,
    win_ref, gain_ref, colsum_ref, wsrc_ref, wout_ref, x_buf, b_buf, pool_ref, res_src, res_in, acc, s1, s2, own_sum, ctx_in, sums_out, sums_in, stage,
    local_sem, ws, wr, xs, xr, cs, cr, ps, pr, rs, rr,
):
    s = lax.axis_index("section")
    me = lax.axis_index("tp")
    z, y = me // ny, me % ny
    nxt, prv = (s + 1) % sections, (s + sections - 1) % sections
    devices = nz * ny
    rows, width = x_buf.shape[2], x_buf.shape[3]
    half = rows // 2
    cols = win_ref.shape[1] // 3
    group = ny * width
    lost = lost_ref[0]

    def at(dz, dy):
        return ((z + dz) % nz) * ny + (y + dy) % ny

    def row_of(dz):
        return (z + dz) % nz

    def copy_to(src, dst, send, recv, section, tp):
        return pltpu.make_async_remote_copy(
            src_ref=src, dst_ref=dst, send_sem=send, recv_sem=recv,
            device_id={"section": section, "tp": tp}, device_id_type=MESH,
        )

    def local(src, dst, i):
        return pltpu.make_async_copy(src, dst, local_sem.at[i])

    def pick(cond, a, b):
        return jnp.where(jnp.full(a.shape, cond), a, b)

    def runs(section, n):
        idle = (section == 0) & (n == TICKS)
        idle = idle | (((section == 1) | (section == 2)) & (n == TICKS + 1))
        return jnp.logical_not(idle)

    def gathers(section, n):
        return (n > 0) & jnp.logical_not((section == 1) & (n == TICKS + 1))

    local(gain_hbm, gain_ref, 4).start()
    depth = win_ref.shape[0] // 2
    for h in range(2):
        for i in range(3):
            local(win_hbm.at[i, pl.ds(h * depth, depth)], win_ref.at[pl.ds(h * depth, depth), pl.ds(i * cols, cols)], 7 * h).start()
    for j in range(devices):
        local(pend_hbm.at[0, :, pl.ds(j * width, width)], x_buf.at[0, j], 1).start()
    local(wout_hbm, wsrc_ref, 5).start()
    for j in range(nz):
        local(wout_hbm.at[:, pl.ds(pl.multiple_of((j * ny + y) * width, 128), width // 2)],
              wout_ref.at[0, pl.ds(pl.multiple_of(y * cols, 128), cols), pl.ds(j * (width // 2), width // 2)], 6).start()
    local(pool_hbm, pool_ref, 2).start()

    barrier = pltpu.get_barrier_semaphore()
    for dz, dy in PEERS + ((0, 0),):
        pl.semaphore_signal(barrier, inc=1, device_id={"section": prv, "tp": at(dz, dy)}, device_id_type=MESH)
    for dz, dy in PEERS:
        pl.semaphore_signal(barrier, inc=1, device_id={"section": s, "tp": at(dz, dy)}, device_id_type=MESH)

    eye = lax.broadcasted_iota(jnp.int32, (width, width), 0) == lax.broadcasted_iota(jnp.int32, (width, width), 1)
    colsum_ref[...] = jnp.zeros_like(colsum_ref)
    local(gain_hbm, gain_ref, 4).wait()

    def fold(j, carry):
        span = pl.ds(pl.multiple_of(j * width, width), width)
        scale = jnp.where(eye, jnp.broadcast_to(gain_ref[:, span].astype(jnp.float32), (width, width)), 0.0)
        scaled = jnp.dot(scale.astype(jnp.bfloat16), win_ref[span, :], preferred_element_type=jnp.float32)
        scaled = scaled.astype(jnp.bfloat16)
        win_ref[span, :] = scaled
        colsum_ref[...] += jnp.sum(scaled.astype(jnp.float32).reshape(width // 8, 8, 3 * cols), axis=0)
        return carry

    def fold_half(h):
        top = win_ref.at[pl.ds(h * depth, depth)]
        pltpu.make_async_copy(top, top, local_sem.at[7 * h]).wait()
        with jax.named_scope("fold"):
            lax.fori_loop(h * devices // 2, (h + 1) * devices // 2, fold, 0, unroll=4)

    fold_half(0)
    def residual(n, src):
        return copy_to(src, res_in.at[n], rs.at[n], rr.at[n], nxt, me)

    def w_send():
        for k in (2, 1, 3, 0):
            for j in range(ny):
                t = row_of(k) * ny + j
                copy_to(wsrc_ref.at[:, pl.ds(pl.multiple_of(t * width + width // 2, 128), width // 2)],
                        wout_ref.at[1, pl.ds(pl.multiple_of(z * cols, 128), cols), pl.ds(j * (width // 2), width // 2)],
                        ws, wr.at[1], nxt, at(k, 0)).start()
            if k:
                for j in range(nz):
                    t = j * ny + (y + k) % ny
                    copy_to(wsrc_ref.at[:, pl.ds(pl.multiple_of(t * width, 128), width // 2)],
                            wout_ref.at[0, pl.ds(pl.multiple_of(y * cols, 128), cols), pl.ds(j * (width // 2), width // 2)],
                            ws, wr.at[0], s, at(0, k)).start()

    def half_of(h):
        return pl.ds(h * half, half)

    def x_copy(n, h, slot, tp):
        ref = x_buf.at[n, slot, half_of(h)]
        return copy_to(ref, ref, xs.at[n], xr.at[n, h, slot], s, tp)

    def x_send(n):
        for k in NEAR_FIRST:
            x_copy(n, 0, me, at(k, 0)).start()
            x_copy(n, 1, me, at(0, k)).start()
        for k in NEAR_FIRST:
            x_copy(n, 1, me, at(k, 0)).start()
            x_copy(n, 0, me, at(0, k)).start()

    def x_forward(n):
        for k in NEAR_FIRST:
            x_copy(n, 0, at(k, 0), me).wait_recv()
            for m in NEAR_FIRST:
                x_copy(n, 0, at(k, 0), at(0, m)).start()
            x_copy(n, 1, at(0, k), me).wait_recv()
            for m in NEAR_FIRST:
                x_copy(n, 1, at(0, k), at(m, 0)).start()

    def x_settle(n, dz):
        for k in (0,) + NEAR_FIRST:
            if k:
                x_copy(n, 0, at(dz, k), me).wait_recv()
            if dz:
                x_copy(n, 1, at(dz, k), me).wait_recv()

    def c_copy(n, slot, section, tp):
        return copy_to(ctx_in.at[n, y], ctx_in.at[n, slot], cs.at[n], cr.at[n, slot], section, tp)

    def c_send(n):
        for k in (2, 1, 3, 0):
            c_copy(n, ny + z, nxt, at(k, 0)).start()
            if k:
                c_copy(n, y, s, at(0, k)).start()

    def p_copy(n, i, k, j, section, tp):
        return copy_to(sums_out.at[n, i, j], sums_in.at[n, i, k], ps.at[n, i], pr.at[n, i, k], section, tp)

    def partial(n, i):
        heads = jnp.concatenate([ctx_in[n, i * ny + k] for k in range(ny)], axis=1)
        sums = jnp.dot(heads, wout_ref[i], preferred_element_type=jnp.float32)
        for j in range(nz):
            piece = sums[:, j * (width // 2):(j + 1) * (width // 2)]
            if i:
                own_sum[j] = piece
            sums_out[n, i, j] = piece.astype(jnp.bfloat16)

    def spread(n):
        with jax.named_scope("cwait0"):
            for k in NEAR_FIRST:
                c_copy(n, (y + k) % ny, s, me).wait_recv()
        partial(n, 0)
        for k in (2, 1, 3, 0):
            p_copy(n, 0, k, row_of(k), nxt, at(k, 0)).start()

    def layer(n, first):
        def alive(block):
            return pick(s == lost, jnp.zeros_like(block), block) if first else block

        own = alive(x_buf[n, me]).astype(jnp.float32)
        shift = jnp.broadcast_to(jnp.sum(own, axis=-1, keepdims=True) / width, (rows, width))
        for i, dz in enumerate((0,) + NEAR_FIRST):
            if not first:
                with jax.named_scope("xsettle%d" % i):
                    x_settle(n, dz)
            zr = row_of(dz)
            blocks, sums, squares = [], None, None
            for k in range(ny):
                block = alive(x_buf[n, zr * ny + k])
                blocks.append(block)
                moved = block.astype(jnp.float32) - shift
                square = moved * moved
                sums = moved if sums is None else sums + moved
                squares = square if squares is None else squares + square
            wide = jnp.concatenate(blocks, axis=1)
            weights = win_ref[pl.ds(pl.multiple_of(zr * group, group), group), :]
            product = jnp.dot(wide, weights, preferred_element_type=jnp.float32)
            sums = sums[:, :width // 2] + sums[:, width // 2:]
            squares = squares[:, :width // 2] + squares[:, width // 2:]
            if i == 0:
                acc[...] = product
                s1[...] = sums
                s2[...] = squares
            elif i < nz - 1:
                acc[...] += product
                s1[...] += sums
                s2[...] += squares
            else:
                product = acc[...] + product
                sums = s1[...] + sums
                squares = s2[...] + squares
        with jax.named_scope("attend"):
            attend(n, product, sums, squares, shift)

    def attend(n, product, sums, squares, shift):
        count = float(devices * width)
        off = jnp.sum(sums, axis=-1, keepdims=True) / count
        var = jnp.sum(squares, axis=-1, keepdims=True) / count - off * off
        rstd = lax.rsqrt(var + NORM_EPS)
        mean = shift[:, :1] + off
        qkv = ((product - mean * colsum_ref[:1]) * rstd).astype(jnp.bfloat16)
        q, k, v = qkv[:, :HD], qkv[:, HD:2 * HD], qkv[:, 2 * HD:]
        scores = lax.dot_general(q, k, (((1,), (1,)), ((), ())), preferred_element_type=jnp.float32)
        causal = lax.broadcasted_iota(jnp.int32, (rows, rows), 0) >= lax.broadcasted_iota(jnp.int32, (rows, rows), 1)
        scores = jnp.where(causal, scores * HD ** (-0.5), -jnp.inf)
        weights = jnp.exp(scores - jnp.max(scores, axis=-1, keepdims=True))
        probs = (weights / jnp.sum(weights, axis=-1, keepdims=True)).astype(jnp.bfloat16)
        ctx_in[n, y] = jnp.dot(probs, v, preferred_element_type=jnp.float32).astype(jnp.bfloat16)

    def finish(n):
        with jax.named_scope("cwait1"):
            for k in (0,) + NEAR_FIRST:
                c_copy(n, ny + row_of(k), s, me).wait_recv()
        partial(n, 1)
        for k in (2, 1, 3):
            p_copy(n, 1, k, (y + k) % ny, s, at(0, k)).start()
        residual(n, res_src).wait_recv()
        for i in (1, 0):
            at_i = slice(i * (width // 2), (i + 1) * (width // 2))
            total = res_in[n, :, at_i].astype(jnp.float32)
            if i:
                total = total + own_sum[y]
            with jax.named_scope("pwait%d" % i):
                for k in NEAR_FIRST + ((0,) if i == 0 else ()):
                    p_copy(n, i, k, 0, s, me).wait_recv()
            for k in NEAR_FIRST + ((0,) if i == 0 else ()):
                total = total + sums_in[n, i, k].astype(jnp.float32)
            b_buf[n + 1, :, at_i] = total.astype(jnp.bfloat16)

    def advance(n):
        @pl.when(s == 0)
        def _():
            settled = pick(sections - TICKS > lost, b_buf[TICKS], b_buf[TICKS + 1])
            settled = pick(sections - 1 == lost, b_buf[1], settled)
            x_buf[n + 1, me] = pick(n < TICKS, pool_ref[plan_ref[n]], settled)

        @pl.when(s != 0)
        def _():
            x_buf[n + 1, me] = b_buf[n + 1]

        @pl.when(gathers(s, n + 1))
        def _():
            x_send(n + 1)

        @pl.when(runs(s, n + 1))
        def _():
            residual(n + 1, x_buf.at[n + 1, me]).start()

    def output():
        early = (s == 0) | (s < lost) | (s - TICKS > lost)
        for j in range(devices):
            block = pick(early, x_buf[TICKS, j], x_buf[TICKS + 1, j])
            later_hbm[0, :, j * width:(j + 1) * width] = pick(s == lost, jnp.zeros_like(block), block)

    pltpu.make_async_copy(wsrc_ref, wsrc_ref, local_sem.at[5]).wait()
    with jax.named_scope("bwait"):
        pl.semaphore_wait(barrier, 2 * len(PEERS) + 1)
    w_send()
    fold_half(1)
    colsum_ref[...] = jnp.broadcast_to(jnp.sum(colsum_ref[...], axis=0, keepdims=True), colsum_ref.shape)
    pltpu.make_async_copy(x_buf.at[0], x_buf.at[0], local_sem.at[1]).wait()
    own = x_buf[0, me]
    res_src[...] = pick(s == lost, jnp.zeros_like(own), own)
    layer(0, True)
    c_send(0)
    residual(0, res_src).start()
    pltpu.make_async_copy(pool_ref, pool_ref, local_sem.at[2]).wait()
    with jax.named_scope("wwait"):
        took = wout_ref.at[0, pl.ds(0, cols)]
        pltpu.make_async_copy(took, took, local_sem.at[6]).wait()
        took = x_buf.at[0, pl.ds(0, devices * (ny - 1) // 8)]
        pltpu.make_async_copy(took, took, wr.at[0]).wait()
        pltpu.make_async_copy(wout_ref.at[1], wout_ref.at[1], wr.at[1]).wait()

    def step(n, carry):
        @pl.when(gathers(s, n))
        def _():
            with jax.named_scope("xfwd"):
                x_forward(n)

        @pl.when(runs(s, n) & (n > 0))
        def _():
            layer(n, False)
            with jax.named_scope("csend"):
                c_send(n)

        @pl.when(runs(s, n))
        def _():
            with jax.named_scope("spread"):
                spread(n)

        @pl.when(gathers(s, n) & jnp.logical_not(runs(s, n)))
        def _():
            for dz in (0,) + NEAR_FIRST:
                x_settle(n, dz)

        @pl.when(n == WAVES - 1)
        def _():
            with jax.named_scope("output"):
                output()

        @pl.when(runs(prv, n))
        def _():
            with jax.named_scope("finish"):
                finish(n)

        @pl.when(jnp.logical_not(runs(prv, n)))
        def _():
            b_buf[n + 1] = jnp.zeros((rows, width), jnp.bfloat16)

        @pl.when(n < WAVES - 1)
        def _():
            with jax.named_scope("advance"):
                advance(n)

        return carry

    lax.fori_loop(0, WAVES, step, 0)

    settled = pick((s - 2 < lost) | (s - 2 - TICKS + 1 > lost), b_buf[TICKS + 1], b_buf[TICKS + 2])
    settled = pick((s + sections - 2) % sections == lost, b_buf[2], settled)
    last = sections - 2
    wrapped = pick((last < lost) | (last - TICKS + 1 > lost), b_buf[TICKS + 1], b_buf[TICKS + 2])
    wrapped = pick(last == lost, b_buf[2], wrapped)
    settled = pick(s == 0, wrapped, settled)
    standby_ref[0] = pick(s == 1, b_buf[TICKS + 2], settled)

    sent = x_buf.at[0, pl.ds(0, devices * (2 * ny - 1) // 8)]
    pltpu.make_async_copy(sent, sent, ws).wait()

    def drain(n, carry):
        @pl.when(gathers(s, n))
        def _():
            ref = x_buf.at[0, pl.ds(0, devices - 1)]
            pltpu.make_async_copy(ref, ref, xs.at[n]).wait()

        @pl.when(runs(s, n))
        def _():
            ref = ctx_in.at[0, pl.ds(0, nz + ny - 1)]
            pltpu.make_async_copy(ref, ref, cs.at[n]).wait()
            ref = ctx_in.at[0, pl.ds(0, nz)]
            pltpu.make_async_copy(ref, ref, ps.at[n, 0]).wait()
            residual(n, res_src).wait_send()

        @pl.when(runs(prv, n))
        def _():
            ref = ctx_in.at[0, pl.ds(0, ny - 1)]
            pltpu.make_async_copy(ref, ref, ps.at[n, 1]).wait()

        return carry

    with jax.named_scope("drain"):
        lax.fori_loop(0, WAVES, drain, 0)


def solution(mesh):
    sections, devices = mesh.shape["section"], mesh.shape["tp"]
    ny = 1
    while (2 * ny) * (2 * ny) <= devices and devices % (2 * ny) == 0:
        ny *= 2
    nz = devices // ny

    def per_device(pend, pool, plan, lost, win, wout, gain):
        rows, hidden = pend.shape[1], pend.shape[2]
        width = hidden // devices
        cols = win.shape[3]
        win = jnp.transpose(win[0], (1, 0, 2))
        vmem = pl.BlockSpec(memory_space=pltpu.VMEM)
        smem = pl.BlockSpec(memory_space=pltpu.SMEM)
        hbm = pl.BlockSpec(memory_space=pltpu.HBM)
        free = pl.BlockSpec(memory_space=pl.ANY)
        bf = functools.partial(pltpu.VMEM, dtype=jnp.bfloat16)
        f32 = functools.partial(pltpu.VMEM, dtype=jnp.float32)
        dma = pltpu.SemaphoreType.DMA
        return pl.pallas_call(
            functools.partial(relay_kernel, sections, nz, ny),
            out_shape=(
                jax.ShapeDtypeStruct((1, rows, hidden), jnp.bfloat16),
                jax.ShapeDtypeStruct((1, rows, width), jnp.bfloat16),
            ),
            in_specs=[smem, smem, hbm, hbm, hbm, hbm, hbm],
            out_specs=(vmem, vmem),
            scratch_shapes=[
                bf((hidden, 3 * cols)),
                bf(gain.shape),
                f32((8, 3 * cols)),
                bf((cols, hidden)),
                bf((2, ny * cols, nz * width // 2)),
                bf((WAVES, devices, rows, width)),
                bf((WAVES + 1, rows, width)),
                bf(pool.shape),
                bf((rows, width)),
                bf((WAVES, rows, width)),
                f32((rows, 3 * cols)),
                f32((rows, width // 2)),
                f32((rows, width // 2)),
                f32((ny, rows, width // 2)),
                bf((WAVES, nz + ny, rows, cols)),
                bf((WAVES, 2, nz, rows, width // 2)),
                bf((WAVES, 2, nz, rows, width // 2)),
                bf((devices, rows, width)),
                dma((8,)), dma, dma((2,)),
                dma((WAVES,)), dma((WAVES, 2, devices)),
                dma((WAVES,)), dma((WAVES, nz + ny)),
                dma((WAVES, 2)), dma((WAVES, 2, nz)),
                dma((WAVES,)), dma((WAVES,)),
            ],
            compiler_params=pltpu.CompilerParams(
                collective_id=0, has_side_effects=True, vmem_limit_bytes=28 * 1024 * 1024
            ),
        )(lost, *[pltpu.with_memory_space_constraint(a, pltpu.HBM) for a in (plan,)], *[pltpu.with_memory_space_constraint(a, pltpu.HBM) for a in (pend, pool, win, wout[0], gain)])

    placed = (
        P("section", None, None),
        P(None, None, "tp"),
        P(),
        P(),
        P("section", None, None, "tp"),
        P("section", "tp", None),
        P("section", None),
    )
    return jax.shard_map(
        per_device,
        mesh=mesh,
        in_specs=placed,
        out_specs=(P("section", None, None), P("section", None, "tp")),
        check_vma=False,
    )
```

```python
import functools

import jax
import jax.numpy as jnp
from jax import lax
from jax.experimental import pallas as pl
from jax.experimental.pallas import tpu as pltpu
from jax.sharding import PartitionSpec as P

HD = 128
TICKS = 3
NORM_EPS = 1e-05
MESH = pl.DeviceIdType.MESH
WAVES = TICKS + 2
ORDERED = False
GROUPS = (
    ((0, 0), (0, 1), (0, 3), (0, 2)),
    ((1, 0), (3, 0), (1, 1), (1, 3)),
    ((3, 1), (3, 3), (2, 0), (1, 2)),
    ((3, 2), (2, 1), (2, 3), (2, 2)),
)
NEAR_FIRST = (1, 3, 2)
PEERS = tuple((k, 0) for k in NEAR_FIRST) + tuple((0, k) for k in NEAR_FIRST)


def relay_kernel(
    sections, nz, ny,
    lost_ref, plan_ref, pend_hbm, pool_hbm, win_hbm, wout_hbm, gain_hbm,
    later_hbm, standby_ref,
    win_ref, gain_ref, colsum_ref, wsrc_ref, wout_ref, x_buf, b_buf, pool_ref, res_src, res_in, acc, s1, s2, own_sum, ctx_in, sums_out, sums_in,
    local_sem, ws, wr, xs, xr, cs, cr, ps, pr, rs, rr,
):
    s = lax.axis_index("section")
    me = lax.axis_index("tp")
    z, y = me // ny, me % ny
    nxt, prv = (s + 1) % sections, (s + sections - 1) % sections
    devices = nz * ny
    rows, lanes = x_buf.shape[3], x_buf.shape[4]
    width = 2 * lanes
    cols = win_ref.shape[1] // 3
    lost = lost_ref[0]

    def at(dz, dy):
        return ((z + dz) % nz) * ny + (y + dy) % ny

    def row_of(dz):
        return (z + dz) % nz

    def copy_to(src, dst, send, recv, section, tp):
        return pltpu.make_async_remote_copy(
            src_ref=src, dst_ref=dst, send_sem=send, recv_sem=recv,
            device_id={"section": section, "tp": tp}, device_id_type=MESH,
        )

    def local(src, dst, i):
        return pltpu.make_async_copy(src, dst, local_sem.at[i])

    def pick(cond, a, b):
        return jnp.where(jnp.full(a.shape, cond), a, b)

    def runs(section, n):
        idle = (section == 0) & (n == TICKS)
        idle = idle | (((section == 1) | (section == 2)) & (n == TICKS + 1))
        return jnp.logical_not(idle)

    def gathers(section, n):
        return (n > 0) & jnp.logical_not((section == 1) & (n == TICKS + 1))

    barrier = pltpu.get_barrier_semaphore()
    for dz, dy in PEERS + ((0, 0),):
        pl.semaphore_signal(barrier, inc=1, device_id={"section": prv, "tp": at(dz, dy)}, device_id_type=MESH)
    for dz, dy in PEERS:
        pl.semaphore_signal(barrier, inc=1, device_id={"section": s, "tp": at(dz, dy)}, device_id_type=MESH)

    local(gain_hbm, gain_ref, 4).start()
    depth = win_ref.shape[0] // 2
    for h in range(2):
        for i in range(3):
            local(win_hbm.at[i, pl.ds(h * depth, depth)], win_ref.at[pl.ds(h * depth, depth), pl.ds(i * cols, cols)], 7 * h).start()
    for j in range(devices):
        for i in range(2):
            local(pend_hbm.at[0, :, pl.ds(j * width + i * lanes, lanes)], x_buf.at[0, i, j], 1).start()
    local(wout_hbm, wsrc_ref, 5).start()
    for j in range(nz):
        local(wout_hbm.at[:, pl.ds(pl.multiple_of((j * ny + y) * width, 128), lanes)],
              wout_ref.at[0, pl.ds(pl.multiple_of(y * cols, 128), cols), pl.ds(j * (lanes), lanes)], 6).start()
    for i in range(2):
        local(pool_hbm.at[:, :, pl.ds(i * lanes, lanes)], pool_ref.at[i], 2).start()

    eye = lax.broadcasted_iota(jnp.int32, (width, width), 0) == lax.broadcasted_iota(jnp.int32, (width, width), 1)
    colsum_ref[...] = jnp.zeros_like(colsum_ref)
    local(gain_hbm, gain_ref, 4).wait()

    def fold(j, carry):
        span = pl.ds(pl.multiple_of(j * width, width), width)
        scale = jnp.where(eye, jnp.broadcast_to(gain_ref[:, span].astype(jnp.float32), (width, width)), 0.0)
        scaled = jnp.dot(scale.astype(jnp.bfloat16), win_ref[span, :], preferred_element_type=jnp.float32)
        scaled = scaled.astype(jnp.bfloat16)
        win_ref[span, :] = scaled
        colsum_ref[...] += jnp.sum(scaled.astype(jnp.float32).reshape(width // 8, 8, 3 * cols), axis=0)
        return carry

    def fold_half(h):
        top = win_ref.at[pl.ds(h * depth, depth)]
        pltpu.make_async_copy(top, top, local_sem.at[7 * h]).wait()
        with jax.named_scope("fold"):
            lax.fori_loop(h * devices // 2, (h + 1) * devices // 2, fold, 0, unroll=4)

    fold_half(0)
    def residual(n, src):
        return copy_to(src, res_in.at[n], rs.at[n], rr.at[n], nxt, me)

    def w_send():
        for k in (2, 1, 3, 0):
            for j in range(ny):
                t = row_of(k) * ny + j
                copy_to(wsrc_ref.at[:, pl.ds(pl.multiple_of(t * width + lanes, 128), lanes)],
                        wout_ref.at[1, pl.ds(pl.multiple_of(z * cols, 128), cols), pl.ds(j * (lanes), lanes)],
                        ws, wr.at[1], nxt, at(k, 0)).start()
            if k:
                for j in range(nz):
                    t = j * ny + (y + k) % ny
                    copy_to(wsrc_ref.at[:, pl.ds(pl.multiple_of(t * width, 128), lanes)],
                            wout_ref.at[0, pl.ds(pl.multiple_of(y * cols, 128), cols), pl.ds(j * (lanes), lanes)],
                            ws, wr.at[0], s, at(0, k)).start()

    def x_copy(n, i, slot, tp):
        ref = x_buf.at[n, i, slot]
        return copy_to(ref, ref, xs.at[n], xr.at[n, i, slot], s, tp)

    def x_send(n, i, along_z):
        for k in NEAR_FIRST:
            x_copy(n, i, me, at(k, 0) if along_z else at(0, k)).start()

    def x_forward(n):
        for k in NEAR_FIRST:
            x_copy(n, 0, at(k, 0), me).wait_recv()
            for m in NEAR_FIRST:
                x_copy(n, 0, at(k, 0), at(0, m)).start()
            x_copy(n, 1, at(0, k), me).wait_recv()
            for m in NEAR_FIRST:
                x_copy(n, 1, at(0, k), at(m, 0)).start()

    def x_settle(n, group):
        for dz, k in group:
            if k:
                x_copy(n, 0, at(dz, k), me).wait_recv()
            if dz:
                x_copy(n, 1, at(dz, k), me).wait_recv()

    def c_copy(n, slot, section, tp):
        return copy_to(ctx_in.at[n, y], ctx_in.at[n, slot], cs.at[n], cr.at[n, slot], section, tp)

    def c_send(n):
        for k in (2, 1, 3, 0):
            c_copy(n, ny + z, nxt, at(k, 0)).start()
            if k:
                c_copy(n, y, s, at(0, k)).start()

    def p_copy(n, i, k, j, section, tp):
        return copy_to(sums_out.at[n, i, j], sums_in.at[n, i, k], ps.at[n, i], pr.at[n, i, k], section, tp)

    def partial(n, i):
        heads = jnp.concatenate([ctx_in[n, i * ny + k] for k in range(ny)], axis=1)
        sums = jnp.dot(heads, wout_ref[i], preferred_element_type=jnp.float32)
        for j in range(nz):
            piece = sums[:, j * (lanes):(j + 1) * (lanes)]
            if i:
                own_sum[j] = piece
            sums_out[n, i, j] = piece.astype(jnp.bfloat16)

    def spread(n):
        with jax.named_scope("cwait0"):
            for k in NEAR_FIRST:
                c_copy(n, (y + k) % ny, s, me).wait_recv()
        partial(n, 0)
        for k in (2, 1, 3, 0):
            p_copy(n, 0, k, row_of(k), nxt, at(k, 0)).start()

    def layer(n, first):
        def alive(block):
            return pick(s == lost, jnp.zeros_like(block), block) if first else block

        own = alive(x_buf[n, :, me]).astype(jnp.float32)
        shift = jnp.broadcast_to(jnp.sum(own[0] + own[1], axis=-1, keepdims=True) / width, (rows, lanes))
        for i, blocks in enumerate(GROUPS):
            if not first:
                with jax.named_scope("xsettle%d" % i):
                    x_settle(n, blocks)
            product, sums, squares = None, None, None
            for dz, k in blocks:
                slot = at(dz, k)
                halves = [alive(x_buf[n, h, slot]) for h in range(2)]
                for half in halves:
                    moved = half.astype(jnp.float32) - shift
                    square = moved * moved
                    sums = moved if sums is None else sums + moved
                    squares = square if squares is None else squares + square
                weights = win_ref[pl.ds(pl.multiple_of(slot * width, width), width), :]
                term = jnp.dot(jnp.concatenate(halves, axis=1), weights, preferred_element_type=jnp.float32)
                product = term if product is None else product + term
            if i == 0:
                acc[...] = product
                s1[...] = sums
                s2[...] = squares
            elif i < len(GROUPS) - 1:
                acc[...] += product
                s1[...] += sums
                s2[...] += squares
            else:
                product = acc[...] + product
                sums = s1[...] + sums
                squares = s2[...] + squares
        with jax.named_scope("attend"):
            attend(n, product, sums, squares, shift)

    def attend(n, product, sums, squares, shift):
        count = float(devices * width)
        off = jnp.sum(sums, axis=-1, keepdims=True) / count
        var = jnp.sum(squares, axis=-1, keepdims=True) / count - off * off
        rstd = lax.rsqrt(var + NORM_EPS)
        mean = shift[:, :1] + off
        qkv = ((product - mean * colsum_ref[:1]) * rstd).astype(jnp.bfloat16)
        q, k, v = qkv[:, :HD], qkv[:, HD:2 * HD], qkv[:, 2 * HD:]
        scores = lax.dot_general(q, k, (((1,), (1,)), ((), ())), preferred_element_type=jnp.float32)
        causal = lax.broadcasted_iota(jnp.int32, (rows, rows), 0) >= lax.broadcasted_iota(jnp.int32, (rows, rows), 1)
        scores = jnp.where(causal, scores * HD ** (-0.5), -jnp.inf)
        weights = jnp.exp(scores - jnp.max(scores, axis=-1, keepdims=True))
        mixed = jnp.dot(weights.astype(jnp.bfloat16), v, preferred_element_type=jnp.float32)
        ctx_in[n, y] = (mixed / jnp.sum(weights, axis=-1, keepdims=True)).astype(jnp.bfloat16)

    def finish(n):
        with jax.named_scope("cwait1"):
            for k in (0,) + NEAR_FIRST:
                c_copy(n, ny + row_of(k), s, me).wait_recv()
        partial(n, 1)
        for k in (2, 1, 3):
            p_copy(n, 1, k, (y + k) % ny, s, at(0, k)).start()
        residual(n, res_src).wait_recv()

        def total(i):
            base = res_in[n, i].astype(jnp.float32)
            if i:
                base = base + own_sum[y]
            took = NEAR_FIRST + ((0,) if i == 0 else ())
            with jax.named_scope("pwait%d" % i):
                for k in took:
                    p_copy(n, i, k, 0, s, me).wait_recv()
            for k in took:
                base = base + sums_in[n, i, k].astype(jnp.float32)
            b_buf[n + 1, i] = base.astype(jnp.bfloat16)

        def both(order):
            for i in order:
                total(i)

                @pl.when(n < WAVES - 1)
                def _():
                    advance(n, i)

                    @pl.when(gathers(s, n + 1))
                    def _():
                        x_send(n + 1, i, i == 0)

            @pl.when(gathers(s, n + 1) & (n < WAVES - 1))
            def _():
                for i in order:
                    x_send(n + 1, i, i == 1)

        if ORDERED:
            @pl.when(s % 2 == 0)
            def _():
                both((0, 1))

            @pl.when(s % 2 == 1)
            def _():
                both((1, 0))
        else:
            both((1, 0))

        @pl.when(runs(s, n + 1) & (n < WAVES - 1))
        def _():
            residual(n + 1, x_buf.at[n + 1, :, me]).start()

    def advance(n, i):
        @pl.when(s == 0)
        def _():
            settled = pick(sections - TICKS > lost, b_buf[TICKS, i], b_buf[TICKS + 1, i])
            settled = pick(sections - 1 == lost, b_buf[1, i], settled)
            x_buf[n + 1, i, me] = pick(n < TICKS, pool_ref[i, plan_ref[n]], settled)

        @pl.when(s != 0)
        def _():
            x_buf[n + 1, i, me] = b_buf[n + 1, i]

    def output():
        early = (s == 0) | (s < lost) | (s - TICKS > lost)
        for j in range(devices):
            for i in range(2):
                block = pick(early, x_buf[TICKS, i, j], x_buf[TICKS + 1, i, j])
                at_i = slice(j * width + i * lanes, j * width + (i + 1) * lanes)
                later_hbm[0, :, at_i] = pick(s == lost, jnp.zeros_like(block), block)

    pltpu.make_async_copy(wsrc_ref, wsrc_ref, local_sem.at[5]).wait()
    with jax.named_scope("bwait"):
        pl.semaphore_wait(barrier, 2 * len(PEERS) + 1)
    w_send()
    fold_half(1)
    colsum_ref[...] = jnp.broadcast_to(jnp.sum(colsum_ref[...], axis=0, keepdims=True), colsum_ref.shape)
    pltpu.make_async_copy(x_buf.at[0], x_buf.at[0], local_sem.at[1]).wait()
    own = x_buf[0, :, me]
    res_src[...] = pick(s == lost, jnp.zeros_like(own), own)
    layer(0, True)
    c_send(0)
    residual(0, res_src).start()
    pltpu.make_async_copy(pool_ref, pool_ref, local_sem.at[2]).wait()
    with jax.named_scope("wwait"):
        took = wout_ref.at[0, pl.ds(0, cols)]
        pltpu.make_async_copy(took, took, local_sem.at[6]).wait()
        took = x_buf.at[0, 0, pl.ds(0, nz * (ny - 1))]
        pltpu.make_async_copy(took, took, wr.at[0]).wait()
        pltpu.make_async_copy(wout_ref.at[1], wout_ref.at[1], wr.at[1]).wait()

    def step(n, carry):
        @pl.when(gathers(s, n))
        def _():
            with jax.named_scope("xfwd"):
                x_forward(n)

        @pl.when(runs(s, n) & (n > 0))
        def _():
            layer(n, False)
            with jax.named_scope("csend"):
                c_send(n)

        @pl.when(runs(s, n))
        def _():
            with jax.named_scope("spread"):
                spread(n)

        @pl.when(gathers(s, n) & jnp.logical_not(runs(s, n)))
        def _():
            for blocks in GROUPS:
                x_settle(n, blocks)

        @pl.when(n == WAVES - 1)
        def _():
            with jax.named_scope("output"):
                output()

        @pl.when(runs(prv, n))
        def _():
            with jax.named_scope("finish"):
                finish(n)

        @pl.when(jnp.logical_not(runs(prv, n)))
        def _():
            b_buf[n + 1] = jnp.zeros((2, rows, lanes), jnp.bfloat16)

        return carry

    lax.fori_loop(0, WAVES, step, 0)

    settled = pick((s - 2 < lost) | (s - 2 - TICKS + 1 > lost), b_buf[TICKS + 1], b_buf[TICKS + 2])
    settled = pick((s + sections - 2) % sections == lost, b_buf[2], settled)
    last = sections - 2
    wrapped = pick((last < lost) | (last - TICKS + 1 > lost), b_buf[TICKS + 1], b_buf[TICKS + 2])
    wrapped = pick(last == lost, b_buf[2], wrapped)
    settled = pick(s == 0, wrapped, settled)
    settled = pick(s == 1, b_buf[TICKS + 2], settled)
    for i in range(2):
        standby_ref[0, :, i * lanes:(i + 1) * lanes] = settled[i]

    sent = x_buf.at[0:2, 0, pl.ds(0, nz * (2 * ny - 1) // 2)]
    pltpu.make_async_copy(sent, sent, ws).wait()

    def drain(n, carry):
        @pl.when(gathers(s, n))
        def _():
            ref = x_buf.at[0, :, pl.ds(0, devices - 1)]
            pltpu.make_async_copy(ref, ref, xs.at[n]).wait()

        @pl.when(runs(s, n))
        def _():
            ref = ctx_in.at[0, pl.ds(0, nz + ny - 1)]
            pltpu.make_async_copy(ref, ref, cs.at[n]).wait()
            ref = ctx_in.at[0, pl.ds(0, nz)]
            pltpu.make_async_copy(ref, ref, ps.at[n, 0]).wait()
            residual(n, res_src).wait_send()

        @pl.when(runs(prv, n))
        def _():
            ref = ctx_in.at[0, pl.ds(0, ny - 1)]
            pltpu.make_async_copy(ref, ref, ps.at[n, 1]).wait()

        return carry

    with jax.named_scope("drain"):
        lax.fori_loop(0, WAVES, drain, 0)


def solution(mesh):
    sections, devices = mesh.shape["section"], mesh.shape["tp"]
    ny = 1
    while (2 * ny) * (2 * ny) <= devices and devices % (2 * ny) == 0:
        ny *= 2
    nz = devices // ny

    def per_device(pend, pool, plan, lost, win, wout, gain):
        rows, hidden = pend.shape[1], pend.shape[2]
        width = hidden // devices
        cols = win.shape[3]
        win = jnp.transpose(win[0], (1, 0, 2))
        vmem = pl.BlockSpec(memory_space=pltpu.VMEM)
        smem = pl.BlockSpec(memory_space=pltpu.SMEM)
        hbm = pl.BlockSpec(memory_space=pltpu.HBM)
        free = pl.BlockSpec(memory_space=pl.ANY)
        bf = functools.partial(pltpu.VMEM, dtype=jnp.bfloat16)
        f32 = functools.partial(pltpu.VMEM, dtype=jnp.float32)
        dma = pltpu.SemaphoreType.DMA
        return pl.pallas_call(
            functools.partial(relay_kernel, sections, nz, ny),
            out_shape=(
                jax.ShapeDtypeStruct((1, rows, hidden), jnp.bfloat16),
                jax.ShapeDtypeStruct((1, rows, width), jnp.bfloat16),
            ),
            in_specs=[smem, smem, hbm, hbm, hbm, hbm, hbm],
            out_specs=(vmem, vmem),
            scratch_shapes=[
                bf((hidden, 3 * cols)),
                bf(gain.shape),
                f32((8, 3 * cols)),
                bf((cols, hidden)),
                bf((2, ny * cols, nz * width // 2)),
                bf((WAVES, 2, devices, rows, width // 2)),
                bf((WAVES + 1, 2, rows, width // 2)),
                bf((2,) + pool.shape[:2] + (width // 2,)),
                bf((2, rows, width // 2)),
                bf((WAVES, 2, rows, width // 2)),
                f32((rows, 3 * cols)),
                f32((rows, width // 2)),
                f32((rows, width // 2)),
                f32((ny, rows, width // 2)),
                bf((WAVES, nz + ny, rows, cols)),
                bf((WAVES, 2, nz, rows, width // 2)),
                bf((WAVES, 2, nz, rows, width // 2)),
                dma((8,)), dma, dma((2,)),
                dma((WAVES,)), dma((WAVES, 2, devices)),
                dma((WAVES,)), dma((WAVES, nz + ny)),
                dma((WAVES, 2)), dma((WAVES, 2, nz)),
                dma((WAVES,)), dma((WAVES,)),
            ],
            compiler_params=pltpu.CompilerParams(
                collective_id=0, has_side_effects=True, vmem_limit_bytes=28 * 1024 * 1024
            ),
        )(lost, *[pltpu.with_memory_space_constraint(a, pltpu.HBM) for a in (plan,)], *[pltpu.with_memory_space_constraint(a, pltpu.HBM) for a in (pend, pool, win, wout[0], gain)])

    placed = (
        P("section", None, None),
        P(None, None, "tp"),
        P(),
        P(),
        P("section", None, None, "tp"),
        P("section", "tp", None),
        P("section", None),
    )
    return jax.shard_map(
        per_device,
        mesh=mesh,
        in_specs=placed,
        out_specs=(P("section", None, None), P("section", None, "tp")),
        check_vma=False,
    )
```

```python
import functools

import jax
import jax.numpy as jnp
from jax import lax
from jax.experimental import pallas as pl
from jax.experimental.pallas import tpu as pltpu
from jax.sharding import PartitionSpec as P

HD = 128
TICKS = 3
NORM_EPS = 1e-05
MESH = pl.DeviceIdType.MESH
WAVES = TICKS + 2
ORDERED = False
GROUPS = (
    ((0, 0), (0, 1), (0, 3), (0, 2)),
    ((1, 0), (3, 0), (1, 1), (1, 3)),
    ((3, 1), (3, 3), (2, 0), (1, 2)),
    ((3, 2), (2, 1), (2, 3), (2, 2)),
)
NEAR_FIRST = (1, 3, 2)
PEERS = tuple((k, 0) for k in NEAR_FIRST) + tuple((0, k) for k in NEAR_FIRST)


def relay_kernel(
    sections, nz, ny,
    lost_ref, plan_hbm, pend_hbm, pool_hbm, win_hbm, wout_hbm, gain_hbm,
    later_hbm, standby_ref,
    plan_ref, win_ref, gain_ref, colsum_ref, wsrc_ref, wout_ref, x_buf, b_buf, pool_ref, res_src, res_in, acc, s1, s2, own_sum, ctx_in, sums_out, sums_in,
    local_sem, ws, wr, xs, xr, cs, cr, ps, pr, rs, rr,
):
    s = lax.axis_index("section")
    me = lax.axis_index("tp")
    z, y = me // ny, me % ny
    nxt, prv = (s + 1) % sections, (s + sections - 1) % sections
    devices = nz * ny
    rows, lanes = x_buf.shape[3], x_buf.shape[4]
    width = 2 * lanes
    cols = win_ref.shape[1] // 3

    def at(dz, dy):
        return ((z + dz) % nz) * ny + (y + dy) % ny

    def row_of(dz):
        return (z + dz) % nz

    def copy_to(src, dst, send, recv, section, tp):
        return pltpu.make_async_remote_copy(
            src_ref=src, dst_ref=dst, send_sem=send, recv_sem=recv,
            device_id={"section": section, "tp": tp}, device_id_type=MESH,
        )

    def local(src, dst, i):
        return pltpu.make_async_copy(src, dst, local_sem.at[i])

    def pick(cond, a, b):
        return jnp.where(jnp.full(a.shape, cond), a, b)

    def runs(section, n):
        idle = (section == 0) & (n == TICKS)
        idle = idle | (((section == 1) | (section == 2)) & (n == TICKS + 1))
        return jnp.logical_not(idle)

    def gathers(section, n):
        return (n > 0) & jnp.logical_not((section == 1) & (n == TICKS + 1))

    barrier = pltpu.get_barrier_semaphore()
    for dz, dy in PEERS + ((0, 0),):
        pl.semaphore_signal(barrier, inc=1, device_id={"section": prv, "tp": at(dz, dy)}, device_id_type=MESH)
    for dz, dy in PEERS:
        pl.semaphore_signal(barrier, inc=1, device_id={"section": s, "tp": at(dz, dy)}, device_id_type=MESH)

    local(gain_hbm, gain_ref, 4).start()
    local(plan_hbm, plan_ref, 9).start()
    depth = win_ref.shape[0] // 2
    for h in range(2):
        for i in range(3):
            local(win_hbm.at[i, pl.ds(h * depth, depth)], win_ref.at[pl.ds(h * depth, depth), pl.ds(i * cols, cols)], 7 * h).start()
    for j in range(devices):
        for i in range(2):
            local(pend_hbm.at[0, :, pl.ds(j * width + i * lanes, lanes)], x_buf.at[0, i, j], 1).start()
    local(wout_hbm, wsrc_ref, 5).start()
    for j in range(nz):
        local(wout_hbm.at[:, pl.ds(pl.multiple_of((j * ny + y) * width, 128), lanes)],
              wout_ref.at[0, pl.ds(pl.multiple_of(y * cols, 128), cols), pl.ds(j * (lanes), lanes)], 6).start()
    for i in range(2):
        local(pool_hbm.at[:, :, pl.ds(i * lanes, lanes)], pool_ref.at[i], 2).start()

    eye = lax.broadcasted_iota(jnp.int32, (width, width), 0) == lax.broadcasted_iota(jnp.int32, (width, width), 1)
    colsum_ref[...] = jnp.zeros_like(colsum_ref)
    local(gain_hbm, gain_ref, 4).wait()

    def fold(j, carry):
        span = pl.ds(pl.multiple_of(j * width, width), width)
        scale = jnp.where(eye, jnp.broadcast_to(gain_ref[:, span].astype(jnp.float32), (width, width)), 0.0)
        scaled = jnp.dot(scale.astype(jnp.bfloat16), win_ref[span, :], preferred_element_type=jnp.float32)
        scaled = scaled.astype(jnp.bfloat16)
        win_ref[span, :] = scaled
        colsum_ref[...] += jnp.sum(scaled.astype(jnp.float32).reshape(width // 8, 8, 3 * cols), axis=0)
        return carry

    def fold_half(h):
        top = win_ref.at[pl.ds(h * depth, depth)]
        pltpu.make_async_copy(top, top, local_sem.at[7 * h]).wait()
        with jax.named_scope("fold"):
            lax.fori_loop(h * devices // 2, (h + 1) * devices // 2, fold, 0, unroll=4)

    fold_half(0)
    def residual(n, src):
        return copy_to(src, res_in.at[n], rs.at[n], rr.at[n], nxt, me)

    def w_send():
        for k in (2, 1, 3, 0):
            for j in range(ny):
                t = row_of(k) * ny + j
                copy_to(wsrc_ref.at[:, pl.ds(pl.multiple_of(t * width + lanes, 128), lanes)],
                        wout_ref.at[1, pl.ds(pl.multiple_of(z * cols, 128), cols), pl.ds(j * (lanes), lanes)],
                        ws, wr.at[1], nxt, at(k, 0)).start()
            if k:
                for j in range(nz):
                    t = j * ny + (y + k) % ny
                    copy_to(wsrc_ref.at[:, pl.ds(pl.multiple_of(t * width, 128), lanes)],
                            wout_ref.at[0, pl.ds(pl.multiple_of(y * cols, 128), cols), pl.ds(j * (lanes), lanes)],
                            ws, wr.at[0], s, at(0, k)).start()

    def x_copy(n, i, slot, tp):
        ref = x_buf.at[n, i, slot]
        return copy_to(ref, ref, xs.at[n], xr.at[n, i, slot], s, tp)

    def x_send(n, i, along_z):
        for k in NEAR_FIRST:
            x_copy(n, i, me, at(k, 0) if along_z else at(0, k)).start()

    def x_forward(n):
        for k in NEAR_FIRST:
            x_copy(n, 0, at(k, 0), me).wait_recv()
            for m in NEAR_FIRST:
                x_copy(n, 0, at(k, 0), at(0, m)).start()
            x_copy(n, 1, at(0, k), me).wait_recv()
            for m in NEAR_FIRST:
                x_copy(n, 1, at(0, k), at(m, 0)).start()

    def x_settle(n, group):
        for dz, k in group:
            if k:
                x_copy(n, 0, at(dz, k), me).wait_recv()
            if dz:
                x_copy(n, 1, at(dz, k), me).wait_recv()

    def c_copy(n, slot, section, tp):
        return copy_to(ctx_in.at[n, y], ctx_in.at[n, slot], cs.at[n], cr.at[n, slot], section, tp)

    def c_send(n):
        for k in (2, 1, 3, 0):
            c_copy(n, ny + z, nxt, at(k, 0)).start()
            if k:
                c_copy(n, y, s, at(0, k)).start()

    def p_copy(n, i, k, j, section, tp):
        return copy_to(sums_out.at[n, i, j], sums_in.at[n, i, k], ps.at[n, i], pr.at[n, i, k], section, tp)

    def partial(n, i):
        heads = jnp.concatenate([ctx_in[n, i * ny + k] for k in range(ny)], axis=1)
        sums = jnp.dot(heads, wout_ref[i], preferred_element_type=jnp.float32)
        for j in range(nz):
            piece = sums[:, j * (lanes):(j + 1) * (lanes)]
            if i:
                own_sum[j] = piece
            sums_out[n, i, j] = piece.astype(jnp.bfloat16)

    def spread(n):
        with jax.named_scope("cwait0"):
            for k in NEAR_FIRST:
                c_copy(n, (y + k) % ny, s, me).wait_recv()
        partial(n, 0)
        for k in (2, 1, 3, 0):
            p_copy(n, 0, k, row_of(k), nxt, at(k, 0)).start()

    def layer(n, first):
        def alive(block):
            return pick(s == lost, jnp.zeros_like(block), block) if first else block

        own = alive(x_buf[n, :, me]).astype(jnp.float32)
        shift = jnp.broadcast_to(jnp.sum(own[0] + own[1], axis=-1, keepdims=True) / width, (rows, lanes))
        for i, blocks in enumerate(GROUPS):
            if not first:
                with jax.named_scope("xsettle%d" % i):
                    x_settle(n, blocks)
            product, sums, squares = None, None, None
            for dz, k in blocks:
                slot = at(dz, k)
                halves = [alive(x_buf[n, h, slot]) for h in range(2)]
                for half in halves:
                    moved = half.astype(jnp.float32) - shift
                    square = moved * moved
                    sums = moved if sums is None else sums + moved
                    squares = square if squares is None else squares + square
                weights = win_ref[pl.ds(pl.multiple_of(slot * width, width), width), :]
                term = jnp.dot(jnp.concatenate(halves, axis=1), weights, preferred_element_type=jnp.float32)
                product = term if product is None else product + term
            if i == 0:
                acc[...] = product
                s1[...] = sums
                s2[...] = squares
            elif i < len(GROUPS) - 1:
                acc[...] += product
                s1[...] += sums
                s2[...] += squares
            else:
                product = acc[...] + product
                sums = s1[...] + sums
                squares = s2[...] + squares
        with jax.named_scope("attend"):
            attend(n, product, sums, squares, shift)

    def attend(n, product, sums, squares, shift):
        count = float(devices * width)
        off = jnp.sum(sums, axis=-1, keepdims=True) / count
        var = jnp.sum(squares, axis=-1, keepdims=True) / count - off * off
        rstd = lax.rsqrt(var + NORM_EPS)
        mean = shift[:, :1] + off
        qkv = ((product - mean * colsum_ref[:1]) * rstd).astype(jnp.bfloat16)
        q, k, v = qkv[:, :HD], qkv[:, HD:2 * HD], qkv[:, 2 * HD:]
        scores = lax.dot_general(q, k, (((1,), (1,)), ((), ())), preferred_element_type=jnp.float32)
        causal = lax.broadcasted_iota(jnp.int32, (rows, rows), 0) >= lax.broadcasted_iota(jnp.int32, (rows, rows), 1)
        scores = jnp.where(causal, scores * HD ** (-0.5), -jnp.inf)
        weights = jnp.exp(scores - jnp.max(scores, axis=-1, keepdims=True))
        mixed = jnp.dot(weights.astype(jnp.bfloat16), v, preferred_element_type=jnp.float32)
        ctx_in[n, y] = (mixed / jnp.sum(weights, axis=-1, keepdims=True)).astype(jnp.bfloat16)

    def finish(n):
        with jax.named_scope("cwait1"):
            for k in (0,) + NEAR_FIRST:
                c_copy(n, ny + row_of(k), s, me).wait_recv()
        partial(n, 1)
        for k in (2, 1, 3):
            p_copy(n, 1, k, (y + k) % ny, s, at(0, k)).start()
        residual(n, res_src).wait_recv()

        def total(i):
            base = res_in[n, i].astype(jnp.float32)
            if i:
                base = base + own_sum[y]
            took = NEAR_FIRST + ((0,) if i == 0 else ())
            with jax.named_scope("pwait%d" % i):
                for k in took:
                    p_copy(n, i, k, 0, s, me).wait_recv()
            for k in took:
                base = base + sums_in[n, i, k].astype(jnp.float32)
            b_buf[n + 1, i] = base.astype(jnp.bfloat16)

        def both(order):
            for i in order:
                total(i)

                @pl.when(n < WAVES - 1)
                def _():
                    advance(n, i)

                    @pl.when(gathers(s, n + 1))
                    def _():
                        x_send(n + 1, i, i == 0)

            @pl.when(gathers(s, n + 1) & (n < WAVES - 1))
            def _():
                for i in order:
                    x_send(n + 1, i, i == 1)

        if ORDERED:
            @pl.when(s % 2 == 0)
            def _():
                both((0, 1))

            @pl.when(s % 2 == 1)
            def _():
                both((1, 0))
        else:
            both((1, 0))

        @pl.when(runs(s, n + 1) & (n < WAVES - 1))
        def _():
            residual(n + 1, x_buf.at[n + 1, :, me]).start()

    def advance(n, i):
        @pl.when(s == 0)
        def _():
            settled = pick(sections - TICKS > lost, b_buf[TICKS, i], b_buf[TICKS + 1, i])
            settled = pick(sections - 1 == lost, b_buf[1, i], settled)
            x_buf[n + 1, i, me] = pick(n < TICKS, pool_ref[i, plan_ref[n]], settled)

        @pl.when(s != 0)
        def _():
            x_buf[n + 1, i, me] = b_buf[n + 1, i]

    def output():
        early = (s == 0) | (s < lost) | (s - TICKS > lost)
        for j in range(devices):
            for i in range(2):
                block = pick(early, x_buf[TICKS, i, j], x_buf[TICKS + 1, i, j])
                at_i = slice(j * width + i * lanes, j * width + (i + 1) * lanes)
                later_hbm[0, :, at_i] = pick(s == lost, jnp.zeros_like(block), block)

    pltpu.make_async_copy(wsrc_ref, wsrc_ref, local_sem.at[5]).wait()
    with jax.named_scope("bwait"):
        pl.semaphore_wait(barrier, 2 * len(PEERS) + 1)
    w_send()
    fold_half(1)
    colsum_ref[...] = jnp.broadcast_to(jnp.sum(colsum_ref[...], axis=0, keepdims=True), colsum_ref.shape)
    pltpu.make_async_copy(x_buf.at[0], x_buf.at[0], local_sem.at[1]).wait()
    local(plan_hbm, plan_ref, 9).wait()
    lost = lost_ref[0]
    own = x_buf[0, :, me]
    res_src[...] = pick(s == lost, jnp.zeros_like(own), own)
    layer(0, True)
    c_send(0)
    residual(0, res_src).start()
    pltpu.make_async_copy(pool_ref, pool_ref, local_sem.at[2]).wait()
    with jax.named_scope("wwait"):
        took = wout_ref.at[0, pl.ds(0, cols)]
        pltpu.make_async_copy(took, took, local_sem.at[6]).wait()
        took = x_buf.at[0, 0, pl.ds(0, nz * (ny - 1))]
        pltpu.make_async_copy(took, took, wr.at[0]).wait()
        pltpu.make_async_copy(wout_ref.at[1], wout_ref.at[1], wr.at[1]).wait()

    def step(n, carry):
        @pl.when(gathers(s, n))
        def _():
            with jax.named_scope("xfwd"):
                x_forward(n)

        @pl.when(runs(s, n) & (n > 0))
        def _():
            layer(n, False)
            with jax.named_scope("csend"):
                c_send(n)

        @pl.when(runs(s, n))
        def _():
            with jax.named_scope("spread"):
                spread(n)

        @pl.when(gathers(s, n) & jnp.logical_not(runs(s, n)))
        def _():
            for blocks in GROUPS:
                x_settle(n, blocks)

        @pl.when(n == WAVES - 1)
        def _():
            with jax.named_scope("output"):
                output()

        @pl.when(runs(prv, n))
        def _():
            with jax.named_scope("finish"):
                finish(n)

        @pl.when(jnp.logical_not(runs(prv, n)))
        def _():
            b_buf[n + 1] = jnp.zeros((2, rows, lanes), jnp.bfloat16)

        return carry

    lax.fori_loop(0, WAVES, step, 0)

    settled = pick((s - 2 < lost) | (s - 2 - TICKS + 1 > lost), b_buf[TICKS + 1], b_buf[TICKS + 2])
    settled = pick((s + sections - 2) % sections == lost, b_buf[2], settled)
    last = sections - 2
    wrapped = pick((last < lost) | (last - TICKS + 1 > lost), b_buf[TICKS + 1], b_buf[TICKS + 2])
    wrapped = pick(last == lost, b_buf[2], wrapped)
    settled = pick(s == 0, wrapped, settled)
    settled = pick(s == 1, b_buf[TICKS + 2], settled)
    for i in range(2):
        standby_ref[0, :, i * lanes:(i + 1) * lanes] = settled[i]

    sent = x_buf.at[0:2, 0, pl.ds(0, nz * (2 * ny - 1) // 2)]
    pltpu.make_async_copy(sent, sent, ws).wait()

    def drain(n, carry):
        @pl.when(gathers(s, n))
        def _():
            ref = x_buf.at[0, :, pl.ds(0, devices - 1)]
            pltpu.make_async_copy(ref, ref, xs.at[n]).wait()

        @pl.when(runs(s, n))
        def _():
            ref = ctx_in.at[0, pl.ds(0, nz + ny - 1)]
            pltpu.make_async_copy(ref, ref, cs.at[n]).wait()
            ref = ctx_in.at[0, pl.ds(0, nz)]
            pltpu.make_async_copy(ref, ref, ps.at[n, 0]).wait()
            residual(n, res_src).wait_send()

        @pl.when(runs(prv, n))
        def _():
            ref = ctx_in.at[0, pl.ds(0, ny - 1)]
            pltpu.make_async_copy(ref, ref, ps.at[n, 1]).wait()

        return carry

    with jax.named_scope("drain"):
        lax.fori_loop(0, WAVES, drain, 0)


def solution(mesh):
    sections, devices = mesh.shape["section"], mesh.shape["tp"]
    ny = 1
    while (2 * ny) * (2 * ny) <= devices and devices % (2 * ny) == 0:
        ny *= 2
    nz = devices // ny

    def per_device(pend, pool, plan, lost, win, wout, gain):
        rows, hidden = pend.shape[1], pend.shape[2]
        width = hidden // devices
        cols = win.shape[3]
        win = jnp.transpose(win[0], (1, 0, 2))
        vmem = pl.BlockSpec(memory_space=pltpu.VMEM)
        hbm = pl.BlockSpec(memory_space=pltpu.HBM)
        free = pl.BlockSpec(memory_space=pl.ANY)
        bf = functools.partial(pltpu.VMEM, dtype=jnp.bfloat16)
        f32 = functools.partial(pltpu.VMEM, dtype=jnp.float32)
        dma = pltpu.SemaphoreType.DMA
        return pl.pallas_call(
            functools.partial(relay_kernel, sections, nz, ny),
            out_shape=(
                jax.ShapeDtypeStruct((1, rows, hidden), jnp.bfloat16),
                jax.ShapeDtypeStruct((1, rows, width), jnp.bfloat16),
            ),
            in_specs=[pl.BlockSpec(memory_space=pltpu.SMEM)] + [hbm] * 6,
            out_specs=(vmem, vmem),
            scratch_shapes=[
                pltpu.SMEM(plan.shape, jnp.int32),
                bf((hidden, 3 * cols)),
                bf(gain.shape),
                f32((8, 3 * cols)),
                bf((cols, hidden)),
                bf((2, ny * cols, nz * width // 2)),
                bf((WAVES, 2, devices, rows, width // 2)),
                bf((WAVES + 1, 2, rows, width // 2)),
                bf((2,) + pool.shape[:2] + (width // 2,)),
                bf((2, rows, width // 2)),
                bf((WAVES, 2, rows, width // 2)),
                f32((rows, 3 * cols)),
                f32((rows, width // 2)),
                f32((rows, width // 2)),
                f32((ny, rows, width // 2)),
                bf((WAVES, nz + ny, rows, cols)),
                bf((WAVES, 2, nz, rows, width // 2)),
                bf((WAVES, 2, nz, rows, width // 2)),
                dma((10,)), dma, dma((2,)),
                dma((WAVES,)), dma((WAVES, 2, devices)),
                dma((WAVES,)), dma((WAVES, nz + ny)),
                dma((WAVES, 2)), dma((WAVES, 2, nz)),
                dma((WAVES,)), dma((WAVES,)),
            ],
            compiler_params=pltpu.CompilerParams(
                collective_id=0, has_side_effects=True, vmem_limit_bytes=28 * 1024 * 1024
            ),
        )(lost, *[pltpu.with_memory_space_constraint(a, pltpu.HBM) for a in (plan, pend, pool, win, wout[0], gain)])

    placed = (
        P("section", None, None),
        P(None, None, "tp"),
        P(),
        P(),
        P("section", None, None, "tp"),
        P("section", "tp", None),
        P("section", None),
    )
    return jax.shard_map(
        per_device,
        mesh=mesh,
        in_specs=placed,
        out_specs=(P("section", None, None), P("section", None, "tp")),
        check_vma=False,
    )
```

```python
import functools

import jax
import jax.numpy as jnp
from jax import lax
from jax.experimental import pallas as pl
from jax.experimental.pallas import tpu as pltpu
from jax.sharding import PartitionSpec as P

HD = 128
TICKS = 3
NORM_EPS = 1e-05
MESH = pl.DeviceIdType.MESH
WAVES = TICKS + 2
ORDERED = False
GROUPS = (
    ((0, 0), (0, 1), (0, 3), (0, 2)),
    ((1, 0), (3, 0), (1, 1), (1, 3)),
    ((3, 1), (3, 3), (2, 0), (1, 2)),
    ((3, 2), (2, 1), (2, 3), (2, 2)),
)
NEAR_FIRST = (1, 3, 2)
PEERS = tuple((k, 0) for k in NEAR_FIRST) + tuple((0, k) for k in NEAR_FIRST)


def relay_kernel(
    sections, nz, ny,
    lost_ref, plan_hbm, pend_hbm, pool_hbm, win_hbm, wout_hbm, gain_hbm,
    later_hbm, standby_ref,
    plan_ref, win_ref, gain_ref, colsum_ref, wsrc_ref, wout_ref, x_buf, b_buf, pool_ref, res_src, res_in, acc, s1, s2, own_sum, ctx_in, sums_out, sums_in,
    local_sem, ws, wr, xs, xr, cs, cr, ps, pr, rs, rr,
):
    s = lax.axis_index("section")
    me = lax.axis_index("tp")
    z, y = me // ny, me % ny
    nxt, prv = (s + 1) % sections, (s + sections - 1) % sections
    devices = nz * ny
    rows, lanes = x_buf.shape[3], x_buf.shape[4]
    width = 2 * lanes
    cols = win_ref.shape[1] // 3

    def at(dz, dy):
        return ((z + dz) % nz) * ny + (y + dy) % ny

    def row_of(dz):
        return (z + dz) % nz

    def copy_to(src, dst, send, recv, section, tp):
        return pltpu.make_async_remote_copy(
            src_ref=src, dst_ref=dst, send_sem=send, recv_sem=recv,
            device_id={"section": section, "tp": tp}, device_id_type=MESH,
        )

    def local(src, dst, i):
        return pltpu.make_async_copy(src, dst, local_sem.at[i])

    def pick(cond, a, b):
        return jnp.where(jnp.full(a.shape, cond), a, b)

    def runs(section, n):
        idle = (section == 0) & (n == TICKS)
        idle = idle | (((section == 1) | (section == 2)) & (n == TICKS + 1))
        return jnp.logical_not(idle)

    def gathers(section, n):
        return (n > 0) & jnp.logical_not((section == 1) & (n == TICKS + 1))

    barrier = pltpu.get_barrier_semaphore()
    for dz, dy in PEERS + ((0, 0),):
        pl.semaphore_signal(barrier, inc=1, device_id={"section": prv, "tp": at(dz, dy)}, device_id_type=MESH)
    for dz, dy in PEERS:
        pl.semaphore_signal(barrier, inc=1, device_id={"section": s, "tp": at(dz, dy)}, device_id_type=MESH)

    local(gain_hbm, gain_ref, 4).start()
    local(plan_hbm, plan_ref, 9).start()
    depth = win_ref.shape[0] // 2
    for h in range(2):
        for i in range(3):
            local(win_hbm.at[i, pl.ds(h * depth, depth)], win_ref.at[pl.ds(h * depth, depth), pl.ds(i * cols, cols)], 7 * h).start()
    for j in range(devices):
        for i in range(2):
            local(pend_hbm.at[0, :, pl.ds(j * width + i * lanes, lanes)], x_buf.at[0, i, j], 1).start()
    local(wout_hbm, wsrc_ref, 5).start()
    for j in range(nz):
        local(wout_hbm.at[:, pl.ds(pl.multiple_of((j * ny + y) * width, 128), lanes)],
              wout_ref.at[0, pl.ds(pl.multiple_of(y * cols, 128), cols), pl.ds(j * (lanes), lanes)], 6).start()
    for i in range(2):
        local(pool_hbm.at[:, :, pl.ds(i * lanes, lanes)], pool_ref.at[i], 2).start()

    eye = lax.broadcasted_iota(jnp.int32, (width, width), 0) == lax.broadcasted_iota(jnp.int32, (width, width), 1)
    colsum_ref[...] = jnp.zeros_like(colsum_ref)
    local(gain_hbm, gain_ref, 4).wait()

    def fold(j, carry):
        span = pl.ds(pl.multiple_of(j * width, width), width)
        scale = jnp.where(eye, jnp.broadcast_to(gain_ref[:, span].astype(jnp.float32), (width, width)), 0.0)
        scaled = jnp.dot(scale.astype(jnp.bfloat16), win_ref[span, :], preferred_element_type=jnp.float32)
        scaled = scaled.astype(jnp.bfloat16)
        win_ref[span, :] = scaled
        colsum_ref[...] += jnp.sum(scaled.astype(jnp.float32).reshape(width // 8, 8, 3 * cols), axis=0)
        return carry

    def fold_half(h):
        top = win_ref.at[pl.ds(h * depth, depth)]
        pltpu.make_async_copy(top, top, local_sem.at[7 * h]).wait()
        with jax.named_scope("fold"):
            lax.fori_loop(h * devices // 2, (h + 1) * devices // 2, fold, 0, unroll=4)

    fold_half(0)
    def residual(n, src):
        return copy_to(src, res_in.at[n], rs.at[n], rr.at[n], nxt, me)

    def w_send():
        for k in (2, 1, 3, 0):
            for j in range(ny):
                t = row_of(k) * ny + j
                copy_to(wsrc_ref.at[:, pl.ds(pl.multiple_of(t * width + lanes, 128), lanes)],
                        wout_ref.at[1, pl.ds(pl.multiple_of(z * cols, 128), cols), pl.ds(j * (lanes), lanes)],
                        ws, wr.at[1], nxt, at(k, 0)).start()
            if k:
                for j in range(nz):
                    t = j * ny + (y + k) % ny
                    copy_to(wsrc_ref.at[:, pl.ds(pl.multiple_of(t * width, 128), lanes)],
                            wout_ref.at[0, pl.ds(pl.multiple_of(y * cols, 128), cols), pl.ds(j * (lanes), lanes)],
                            ws, wr.at[0], s, at(0, k)).start()

    def x_copy(n, i, slot, tp):
        ref = x_buf.at[n, i, slot]
        return copy_to(ref, ref, xs.at[n], xr.at[n, i, slot], s, tp)

    def x_send(n, i, along_z):
        for k in NEAR_FIRST:
            x_copy(n, i, me, at(k, 0) if along_z else at(0, k)).start()

    def x_forward(n):
        for k in NEAR_FIRST:
            x_copy(n, 0, at(k, 0), me).wait_recv()
            for m in (NEAR_FIRST if k != 2 else (2, 1, 3)):
                x_copy(n, 0, at(k, 0), at(0, m)).start()
            x_copy(n, 1, at(0, k), me).wait_recv()
            for m in (NEAR_FIRST if k != 2 else (2, 1, 3)):
                x_copy(n, 1, at(0, k), at(m, 0)).start()

    def x_settle(n, group):
        for dz, k in group:
            if k:
                x_copy(n, 0, at(dz, k), me).wait_recv()
            if dz:
                x_copy(n, 1, at(dz, k), me).wait_recv()

    def c_copy(n, slot, section, tp):
        return copy_to(ctx_in.at[n, y], ctx_in.at[n, slot], cs.at[n], cr.at[n, slot], section, tp)

    def c_send(n):
        for k in (2, 1, 3, 0):
            c_copy(n, ny + z, nxt, at(k, 0)).start()
            if k:
                c_copy(n, y, s, at(0, k)).start()

    def p_copy(n, i, k, j, section, tp):
        return copy_to(sums_out.at[n, i, j], sums_in.at[n, i, k], ps.at[n, i], pr.at[n, i, k], section, tp)

    def partial(n, i):
        heads = jnp.concatenate([ctx_in[n, i * ny + k] for k in range(ny)], axis=1)
        sums = jnp.dot(heads, wout_ref[i], preferred_element_type=jnp.float32)
        for j in range(nz):
            piece = sums[:, j * (lanes):(j + 1) * (lanes)]
            if i:
                own_sum[j] = piece
            sums_out[n, i, j] = piece.astype(jnp.bfloat16)

    def spread(n):
        with jax.named_scope("cwait0"):
            for k in NEAR_FIRST:
                c_copy(n, (y + k) % ny, s, me).wait_recv()
        partial(n, 0)
        for k in (2, 1, 3, 0):
            p_copy(n, 0, k, row_of(k), nxt, at(k, 0)).start()

    def layer(n, first):
        def alive(block):
            return pick(s == lost, jnp.zeros_like(block), block) if first else block

        own = alive(x_buf[n, :, me]).astype(jnp.float32)
        shift = jnp.broadcast_to(jnp.sum(own[0] + own[1], axis=-1, keepdims=True) / width, (rows, lanes))
        for i, blocks in enumerate(GROUPS):
            if not first:
                with jax.named_scope("xsettle%d" % i):
                    x_settle(n, blocks)
            product, sums, squares = None, None, None
            for dz, k in blocks:
                slot = at(dz, k)
                halves = [alive(x_buf[n, h, slot]) for h in range(2)]
                for half in halves:
                    moved = half.astype(jnp.float32) - shift
                    square = moved * moved
                    sums = moved if sums is None else sums + moved
                    squares = square if squares is None else squares + square
                weights = win_ref[pl.ds(pl.multiple_of(slot * width, width), width), :]
                term = jnp.dot(jnp.concatenate(halves, axis=1), weights, preferred_element_type=jnp.float32)
                product = term if product is None else product + term
            if i == 0:
                acc[...] = product
                s1[...] = sums
                s2[...] = squares
            elif i < len(GROUPS) - 1:
                acc[...] += product
                s1[...] += sums
                s2[...] += squares
            else:
                product = acc[...] + product
                sums = s1[...] + sums
                squares = s2[...] + squares
        with jax.named_scope("attend"):
            attend(n, product, sums, squares, shift)

    def attend(n, product, sums, squares, shift):
        count = float(devices * width)
        off = jnp.sum(sums, axis=-1, keepdims=True) / count
        var = jnp.sum(squares, axis=-1, keepdims=True) / count - off * off
        rstd = lax.rsqrt(var + NORM_EPS)
        mean = shift[:, :1] + off
        qkv = ((product - mean * colsum_ref[:1]) * rstd).astype(jnp.bfloat16)
        q, k, v = qkv[:, :HD], qkv[:, HD:2 * HD], qkv[:, 2 * HD:]
        scores = lax.dot_general(q, k, (((1,), (1,)), ((), ())), preferred_element_type=jnp.float32)
        causal = lax.broadcasted_iota(jnp.int32, (rows, rows), 0) >= lax.broadcasted_iota(jnp.int32, (rows, rows), 1)
        scores = jnp.where(causal, scores * HD ** (-0.5), -jnp.inf)
        weights = jnp.exp(scores - jnp.max(scores, axis=-1, keepdims=True))
        mixed = jnp.dot(weights.astype(jnp.bfloat16), v, preferred_element_type=jnp.float32)
        ctx_in[n, y] = (mixed / jnp.sum(weights, axis=-1, keepdims=True)).astype(jnp.bfloat16)

    def finish(n):
        with jax.named_scope("cwait1"):
            for k in (0,) + NEAR_FIRST:
                c_copy(n, ny + row_of(k), s, me).wait_recv()
        partial(n, 1)
        for k in (2, 1, 3):
            p_copy(n, 1, k, (y + k) % ny, s, at(0, k)).start()
        residual(n, res_src).wait_recv()

        def total(i):
            base = res_in[n, i].astype(jnp.float32)
            if i:
                base = base + own_sum[y]
            took = NEAR_FIRST + ((0,) if i == 0 else ())
            with jax.named_scope("pwait%d" % i):
                for k in took:
                    p_copy(n, i, k, 0, s, me).wait_recv()
            for k in took:
                base = base + sums_in[n, i, k].astype(jnp.float32)
            b_buf[n + 1, i] = base.astype(jnp.bfloat16)

        def both(order):
            for i in order:
                total(i)

                @pl.when(n < WAVES - 1)
                def _():
                    advance(n, i)

                    @pl.when(gathers(s, n + 1))
                    def _():
                        x_send(n + 1, i, i == 0)

            @pl.when(gathers(s, n + 1) & (n < WAVES - 1))
            def _():
                for i in order:
                    x_send(n + 1, i, i == 1)

        if ORDERED:
            @pl.when(s % 2 == 0)
            def _():
                both((0, 1))

            @pl.when(s % 2 == 1)
            def _():
                both((1, 0))
        else:
            both((1, 0))

        @pl.when(runs(s, n + 1) & (n < WAVES - 1))
        def _():
            residual(n + 1, x_buf.at[n + 1, :, me]).start()

    def advance(n, i):
        @pl.when(s == 0)
        def _():
            settled = pick(sections - TICKS > lost, b_buf[TICKS, i], b_buf[TICKS + 1, i])
            settled = pick(sections - 1 == lost, b_buf[1, i], settled)
            x_buf[n + 1, i, me] = pick(n < TICKS, pool_ref[i, plan_ref[n]], settled)

        @pl.when(s != 0)
        def _():
            x_buf[n + 1, i, me] = b_buf[n + 1, i]

    def output():
        early = (s == 0) | (s < lost) | (s - TICKS > lost)
        for j in range(devices):
            for i in range(2):
                block = pick(early, x_buf[TICKS, i, j], x_buf[TICKS + 1, i, j])
                at_i = slice(j * width + i * lanes, j * width + (i + 1) * lanes)
                later_hbm[0, :, at_i] = pick(s == lost, jnp.zeros_like(block), block)

    pltpu.make_async_copy(wsrc_ref, wsrc_ref, local_sem.at[5]).wait()
    with jax.named_scope("bwait"):
        pl.semaphore_wait(barrier, 2 * len(PEERS) + 1)
    w_send()
    fold_half(1)
    colsum_ref[...] = jnp.broadcast_to(jnp.sum(colsum_ref[...], axis=0, keepdims=True), colsum_ref.shape)
    pltpu.make_async_copy(x_buf.at[0], x_buf.at[0], local_sem.at[1]).wait()
    local(plan_hbm, plan_ref, 9).wait()
    lost = lost_ref[0]
    own = x_buf[0, :, me]
    res_src[...] = pick(s == lost, jnp.zeros_like(own), own)
    layer(0, True)
    c_send(0)
    residual(0, res_src).start()
    pltpu.make_async_copy(pool_ref, pool_ref, local_sem.at[2]).wait()
    with jax.named_scope("wwait"):
        took = wout_ref.at[0, pl.ds(0, cols)]
        pltpu.make_async_copy(took, took, local_sem.at[6]).wait()
        took = x_buf.at[0, 0, pl.ds(0, nz * (ny - 1))]
        pltpu.make_async_copy(took, took, wr.at[0]).wait()
        pltpu.make_async_copy(wout_ref.at[1], wout_ref.at[1], wr.at[1]).wait()

    def step(n, carry):
        @pl.when(gathers(s, n))
        def _():
            with jax.named_scope("xfwd"):
                x_forward(n)

        @pl.when(runs(s, n) & (n > 0))
        def _():
            layer(n, False)
            with jax.named_scope("csend"):
                c_send(n)

        @pl.when(runs(s, n))
        def _():
            with jax.named_scope("spread"):
                spread(n)

        @pl.when(gathers(s, n) & jnp.logical_not(runs(s, n)))
        def _():
            for blocks in GROUPS:
                x_settle(n, blocks)

        @pl.when(n == WAVES - 1)
        def _():
            with jax.named_scope("output"):
                output()

        @pl.when(runs(prv, n))
        def _():
            with jax.named_scope("finish"):
                finish(n)

        @pl.when(jnp.logical_not(runs(prv, n)))
        def _():
            b_buf[n + 1] = jnp.zeros((2, rows, lanes), jnp.bfloat16)

        return carry

    lax.fori_loop(0, WAVES, step, 0)

    settled = pick((s - 2 < lost) | (s - 2 - TICKS + 1 > lost), b_buf[TICKS + 1], b_buf[TICKS + 2])
    settled = pick((s + sections - 2) % sections == lost, b_buf[2], settled)
    last = sections - 2
    wrapped = pick((last < lost) | (last - TICKS + 1 > lost), b_buf[TICKS + 1], b_buf[TICKS + 2])
    wrapped = pick(last == lost, b_buf[2], wrapped)
    settled = pick(s == 0, wrapped, settled)
    settled = pick(s == 1, b_buf[TICKS + 2], settled)
    for i in range(2):
        standby_ref[0, :, i * lanes:(i + 1) * lanes] = settled[i]

    sent = x_buf.at[0:2, 0, pl.ds(0, nz * (2 * ny - 1) // 2)]
    pltpu.make_async_copy(sent, sent, ws).wait()

    def drain(n, carry):
        @pl.when(gathers(s, n))
        def _():
            ref = x_buf.at[0, :, pl.ds(0, devices - 1)]
            pltpu.make_async_copy(ref, ref, xs.at[n]).wait()

        @pl.when(runs(s, n))
        def _():
            ref = ctx_in.at[0, pl.ds(0, nz + ny - 1)]
            pltpu.make_async_copy(ref, ref, cs.at[n]).wait()
            ref = ctx_in.at[0, pl.ds(0, nz)]
            pltpu.make_async_copy(ref, ref, ps.at[n, 0]).wait()
            residual(n, res_src).wait_send()

        @pl.when(runs(prv, n))
        def _():
            ref = ctx_in.at[0, pl.ds(0, ny - 1)]
            pltpu.make_async_copy(ref, ref, ps.at[n, 1]).wait()

        return carry

    with jax.named_scope("drain"):
        lax.fori_loop(0, WAVES, drain, 0)


def solution(mesh):
    sections, devices = mesh.shape["section"], mesh.shape["tp"]
    ny = 1
    while (2 * ny) * (2 * ny) <= devices and devices % (2 * ny) == 0:
        ny *= 2
    nz = devices // ny

    def per_device(pend, pool, plan, lost, win, wout, gain):
        rows, hidden = pend.shape[1], pend.shape[2]
        width = hidden // devices
        cols = win.shape[3]
        win = jnp.transpose(win[0], (1, 0, 2))
        vmem = pl.BlockSpec(memory_space=pltpu.VMEM)
        hbm = pl.BlockSpec(memory_space=pltpu.HBM)
        free = pl.BlockSpec(memory_space=pl.ANY)
        bf = functools.partial(pltpu.VMEM, dtype=jnp.bfloat16)
        f32 = functools.partial(pltpu.VMEM, dtype=jnp.float32)
        dma = pltpu.SemaphoreType.DMA
        return pl.pallas_call(
            functools.partial(relay_kernel, sections, nz, ny),
            out_shape=(
                jax.ShapeDtypeStruct((1, rows, hidden), jnp.bfloat16),
                jax.ShapeDtypeStruct((1, rows, width), jnp.bfloat16),
            ),
            in_specs=[pl.BlockSpec(memory_space=pltpu.SMEM)] + [hbm] * 6,
            out_specs=(vmem, vmem),
            scratch_shapes=[
                pltpu.SMEM(plan.shape, jnp.int32),
                bf((hidden, 3 * cols)),
                bf(gain.shape),
                f32((8, 3 * cols)),
                bf((cols, hidden)),
                bf((2, ny * cols, nz * width // 2)),
                bf((WAVES, 2, devices, rows, width // 2)),
                bf((WAVES + 1, 2, rows, width // 2)),
                bf((2,) + pool.shape[:2] + (width // 2,)),
                bf((2, rows, width // 2)),
                bf((WAVES, 2, rows, width // 2)),
                f32((rows, 3 * cols)),
                f32((rows, width // 2)),
                f32((rows, width // 2)),
                f32((ny, rows, width // 2)),
                bf((WAVES, nz + ny, rows, cols)),
                bf((WAVES, 2, nz, rows, width // 2)),
                bf((WAVES, 2, nz, rows, width // 2)),
                dma((10,)), dma, dma((2,)),
                dma((WAVES,)), dma((WAVES, 2, devices)),
                dma((WAVES,)), dma((WAVES, nz + ny)),
                dma((WAVES, 2)), dma((WAVES, 2, nz)),
                dma((WAVES,)), dma((WAVES,)),
            ],
            compiler_params=pltpu.CompilerParams(
                collective_id=0, has_side_effects=True, vmem_limit_bytes=28 * 1024 * 1024
            ),
        )(lost, *[pltpu.with_memory_space_constraint(a, pltpu.HBM) for a in (plan, pend, pool, win, wout[0], gain)])

    placed = (
        P("section", None, None),
        P(None, None, "tp"),
        P(),
        P(),
        P("section", None, None, "tp"),
        P("section", "tp", None),
        P("section", None),
    )
    return jax.shard_map(
        per_device,
        mesh=mesh,
        in_specs=placed,
        out_specs=(P("section", None, None), P("section", None, "tp")),
        check_vma=False,
    )
```
